64 devices in a mesh: dp: 4 (over x, y), tp: 16 (over z, core).
Axes of the slice: x: 2, y: 2, z: 8, core: 2. Of those that a mesh axis runs over, the one named last changes fastest.
The devices are a block of a 4x4x8 slice.
Arguments:
- ids: int32 [32, 256], P('dp'), parts along dimension 0
- E: bfloat16 [2048, 4096], P(None, 'tp')
- g: bfloat16 [4096], replicated
- W: bfloat16 [4096, 12288], P(None, 'tp')
- du: bfloat16 [32, 256, 12288], P('dp', None, 'tp'), parts along dimension 0
- dres: bfloat16 [32, 256, 4096], P('dp', 'tp'), parts along dimension 0
Outputs:
- output 1: bfloat16 [32, 256, 12288], P('dp', None, 'tp'), parts along dimension 0
- output 2: bfloat16 [32, 256, 4096], P('dp', 'tp'), parts along dimension 0
- output 3: float32 [8192, 4096], P('dp', 'tp'), parts along dimension 0
- output 4: float32 [16384, 12288], P('dp', 'tp'), parts along dimension 0
- output 5: float32 [16384], P('dp'), parts along dimension 0
There are 4 independent parts. The reference program is written for one: setup_inputs(seed, part) draws one part's arguments, and reference() takes and returns one part's arrays. A program takes and returns all parts, laid end to end along the dimension named above; an argument that names none is the same for every part.
All inputs are finite; a program needn't handle non-finite values.
Results may differ from the reference program's by a relative error of at most 0.00618159.
Values are sent between devices in bfloat16 or wider.
A program may use at most 768 MiB of HBM per device.

```python
import jax
import jax.numpy as jnp
from jax import lax
import math

K = 8
T = 256
V = 2048
D = 4096
FC = 12288
EPS = 1e-6


def setup_inputs(seed: int = 0, part: int = 0) -> dict:
    key = jax.random.key(seed)
    kE, kg, kW, kpart = jax.random.split(key, 4)
    kp = jax.random.fold_in(kpart, part)
    k1, k2, k3, k4, k5, k6 = jax.random.split(kp, 6)
    scale = 1.0 / math.sqrt(K * T)
    dscale = scale * math.sqrt(D / FC)
    wscale = 1.0 / math.sqrt(D)
    E = jax.random.normal(kE, (V, D), jnp.float32).astype(jnp.bfloat16)
    g = (1.0 + 0.4 * jax.random.normal(kg, (D,), jnp.float32)).astype(jnp.bfloat16)
    W = (jax.random.normal(kW, (D, FC), jnp.float32) * wscale).astype(jnp.bfloat16)
    rand_bits = jax.random.bits(jax.random.fold_in(k1, 7), (K, T), jnp.uint32) >> 16
    square_part = (rand_bits * rand_bits) >> 16
    fourth_power = (square_part * square_part) >> 16
    ids = jnp.minimum(((fourth_power * (V >> 6)) >> 10).astype(jnp.int32), V - 1)
    du = (jax.random.normal(k5, (K, T, FC), jnp.float32) * dscale).astype(jnp.bfloat16)
    dres = (jax.random.normal(k6, (K, T, D), jnp.float32) * scale).astype(jnp.bfloat16)
    return dict(ids=ids, E=E, g=g, W=W, du=du, dres=dres)


def reference(ids, E, g, W, du, dres):
    gf = g.astype(jnp.float32)

    def step(carry, inp):
        dE, dW, dg = carry
        idk, duk, dresk = inp
        x = jnp.take(E, idk, axis=0)
        xf = x.astype(jnp.float32)
        rs = lax.rsqrt(jnp.mean(xf * xf, axis=-1, keepdims=True) + EPS)
        nh = xf * rs
        n = (nh * gf).astype(jnp.bfloat16)
        u = jnp.dot(n, W, preferred_element_type=jnp.float32).astype(jnp.bfloat16)
        dn = jnp.dot(duk, W.T, preferred_element_type=jnp.float32)
        gdn = gf * dn
        dx = dresk.astype(jnp.float32) + rs * (gdn - nh * jnp.mean(nh * gdn, axis=-1, keepdims=True))
        dE = dE.at[idk].add(dx)
        dW = dW + jnp.dot(n.T, duk, preferred_element_type=jnp.float32)
        dg = dg + jnp.sum(dn * nh, axis=0)
        return (dE, dW, dg), (u, x)

    init = (jnp.zeros((V, D), jnp.float32), jnp.zeros((D, FC), jnp.float32), jnp.zeros((D,), jnp.float32))
    (dE, dW, dg), (u, x) = lax.scan(step, init, (ids, du, dres))
    return u, x, dE, dW, dg
```

```python
import jax
import jax.numpy as jnp
from jax import lax
from jax.sharding import PartitionSpec as P

EPS = 1e-6


def solution(mesh):
    G = mesh.shape['tp']
    C = 2
    Z = G // C
    f32 = jnp.float32
    bf16 = jnp.bfloat16

    def shift(k):
        return [(z * C + c, ((z + k) % Z) * C + c) for z in range(Z) for c in range(C)]

    swap = [(i, i ^ 1) for i in range(G)]

    def body(ids, E, g, W, du, dres):
        K, T = ids.shape
        N = K * T
        V, DL = E.shape
        D = g.shape[0]
        FL = W.shape[1]
        TL = T // G
        r = lax.axis_index('tp')
        z = r // C
        c = r % C
        gf = g.astype(f32)
        idf = ids.reshape(N)

        xl = jnp.take(E, idf, axis=0)
        x = lax.all_gather(xl, 'tp', axis=0, tiled=False)
        dc = lax.all_to_all(dres.reshape(K, TL, G, DL), 'tp', 2, 0, tiled=False)
        dresc = dc.reshape(G, K, TL, DL).transpose(1, 0, 2, 3).reshape(N, DL)

        duf = du.reshape(N, FL)
        W4 = W.reshape(Z, C, DL, FL)
        Wm = lax.dynamic_index_in_dim(W4, c, 1, False)
        Ws = lax.dynamic_index_in_dim(W4, 1 - c, 1, False)
        du_o = lax.ppermute(duf, 'tp', swap)
        W_o = lax.ppermute(Ws, 'tp', swap)
        duc = jnp.concatenate([duf, du_o], axis=1)
        Wc = jnp.concatenate([Wm, W_o], axis=2)

        H = N // 2

        def part(dist):
            wz = lax.dynamic_index_in_dim(Wc, lax.rem(z + dist + Z, Z), 0, False)
            return jnp.einsum('tf,df->td', duc, wz, preferred_element_type=f32)

        F = Z // 2
        order = [F] + [s * d for d in range(F - 1, 0, -1) for s in (1, -1)] + [0]
        parts = {d: part(d) for d in order}
        parts[-F] = parts[F]
        outs = []
        for h in range(2):
            sl = slice(h * H, (h + 1) * H)
            acc = None
            for s in (1, -1):
                L = F if (s == 1) == (h == 0) else F - 1
                buf = parts[s * L][sl].astype(bf16)
                for k in range(L, 0, -1):
                    buf = lax.ppermute(buf, 'tp', shift(s))
                    if k > 1:
                        buf = buf.astype(f32) + parts[s * (k - 1)][sl]
                buf = buf.astype(f32)
                acc = buf if acc is None else acc + buf
            outs.append(acc + parts[0][sl])
        dn = jnp.concatenate(outs, axis=0)

        xf = x.astype(f32)
        ms = jnp.sum(jnp.sum(xf * xf, axis=2), axis=0) / D
        rs = lax.rsqrt(ms + EPS)
        n = (xf * rs[None, :, None] * gf.reshape(G, 1, DL)).astype(bf16)
        n2 = n.transpose(1, 0, 2).reshape(N, D)
        u = jnp.dot(n2, W, preferred_element_type=f32).astype(bf16).reshape(K, T, FL)
        dW = jnp.einsum('td,tf->df', n2, duf, preferred_element_type=f32)
        xt = lax.dynamic_slice_in_dim(x.reshape(G, K, T, DL), r * TL, TL, axis=2)
        xo = xt.transpose(1, 2, 0, 3).reshape(K, TL, D)

        gl = lax.dynamic_slice_in_dim(gf, r * DL, DL)
        nh = xl.astype(f32) * rs[:, None]
        gdn = gl * dn
        sp = jnp.sum(nh * gdn, axis=1)
        dgl = jnp.sum(dn * nh, axis=0)
        small = lax.all_gather(jnp.concatenate([sp, dgl]), 'tp', axis=0)
        s = jnp.sum(small[:, :N], axis=0) / D
        dg = small[:, N:].reshape(D)
        dx = dresc.astype(f32) + rs[:, None] * (gdn - nh * s[:, None])
        hi = dx.astype(bf16)
        r1 = dx - hi.astype(f32)
        mi = r1.astype(bf16)
        lo = (r1 - mi.astype(f32)).astype(bf16)
        onehot = (jnp.arange(V, dtype=jnp.int32)[:, None] == idf[None, :]).astype(bf16)
        d3 = jnp.dot(onehot, jnp.concatenate([hi, mi, lo], axis=1), preferred_element_type=f32)
        dE = d3[:, :DL] + d3[:, DL:2 * DL] + d3[:, 2 * DL:]
        return u, xo, dE, dW, dg

    return jax.shard_map(
        body,
        mesh=mesh,
        in_specs=(P('dp', None), P(None, 'tp'), P(), P(None, 'tp'), P('dp', None, 'tp'), P('dp', 'tp', None)),
        out_specs=(P('dp', None, 'tp'), P('dp', 'tp', None), P('dp', 'tp'), P('dp', 'tp'), P('dp')),
        check_vma=False,
    )
```

```python
import functools

import jax
import jax.numpy as jnp
from jax import lax
from jax.experimental import pallas as pl
from jax.experimental.pallas import tpu as pltpu
from jax.sharding import PartitionSpec as P


EPS = 1e-6
MESH = pl.DeviceIdType.MESH
f32 = jnp.float32
bf16 = jnp.bfloat16


def exchange_kernel(G, s_ref, o_ref, send, recv):
    me = lax.axis_index('tp')
    bar = pltpu.get_barrier_semaphore()
    for k in range(1, G):
        pl.semaphore_signal(bar, inc=1, device_id={'tp': lax.rem(me + k, G)}, device_id_type=MESH)
    pl.semaphore_wait(bar, G - 1)
    copies = []
    for k in range(1, G):
        cp = pltpu.make_async_remote_copy(
            src_ref=s_ref, dst_ref=o_ref.at[me], send_sem=send.at[k - 1], recv_sem=recv.at[k - 1],
            device_id={'tp': lax.rem(me + k, G)}, device_id_type=MESH)
        cp.start()
        copies.append(cp)
    o_ref[me] = s_ref[...]
    for cp in copies:
        cp.wait()


def exchange(G, small):
    rows, lanes = small.shape
    return pl.pallas_call(
        functools.partial(exchange_kernel, G),
        out_shape=jax.ShapeDtypeStruct((G, rows, lanes), small.dtype),
        in_specs=[pl.BlockSpec(memory_space=pltpu.VMEM)],
        out_specs=pl.BlockSpec(memory_space=pltpu.VMEM),
        scratch_shapes=[pltpu.SemaphoreType.DMA((G - 1,)), pltpu.SemaphoreType.DMA((G - 1,))],
        compiler_params=pltpu.CompilerParams(collective_id=0, has_side_effects=True),
        name="exchange",
    )(small)


def forward_kernel(last, DP, *refs):
    if last:
        (eb_ref, rs_ref, g_ref, w_ref, dh_ref, dl_ref, sr_ref, up_ref, ids_ref, _,
         dw_ref, xo_ref, u_ref, acc_ref, ub_ref) = refs
    else:
        (eb_ref, rs_ref, g_ref, w_ref, dh_ref, dl_ref, sr_ref, dw_ref, xo_ref, acc_ref) = refs
    j = pl.program_id(0)
    x = jnp.concatenate([eb_ref[i, 0] for i in range(DP)], axis=1)
    n = (x.astype(f32) * rs_ref[...] * g_ref[...]).astype(bf16)
    dw_ref[...] = (jnp.dot(n, dh_ref[...], preferred_element_type=f32)
                   + jnp.dot(n, dl_ref[...], preferred_element_type=f32))
    xo_ref[...] = lax.dot_general(sr_ref[...], x, (((1,), (1,)), ((), ())),
                                  preferred_element_type=f32).astype(bf16)
    up = lax.dot_general(w_ref[...], n, (((0,), (0,)), ((), ())), preferred_element_type=f32)

    @pl.when(j == 0)
    def _():
        acc_ref[...] = up + up_ref[...] if last else up

    @pl.when(j > 0)
    def _():
        acc_ref[...] += up

    if last:
        @pl.when(j == pl.num_programs(0) - 1)
        def _():
            ub_ref[...] = acc_ref[...].astype(bf16)
            tb = 512

            def step(i, carry):
                rows = pl.ds(pl.multiple_of(i * tb, tb), tb)
                V = ub_ref.shape[1]
                hot = lax.broadcasted_iota(jnp.int32, (tb, V), 1) == ids_ref[rows, :]
                s = jnp.where(hot, 1.0, 0.0).astype(bf16)
                u_ref[rows, :] = lax.dot_general(s, ub_ref[...], (((1,), (1,)), ((), ())),
                                                 preferred_element_type=f32).astype(bf16)
                return carry

            lax.fori_loop(0, u_ref.shape[0] // tb, step, 0)


def forward(q, eb, rs, gcol, W, dh, dl, sr, up=None, ids=None, dw=None):
    last = q == 1
    DP, C, _, Vp = eb.shape
    V = DP * Vp
    D, FL = W.shape
    Dq = D // (2 * C)
    kt = 512
    nk = Dq // kt
    TS = sr.shape[0]
    base = q * C * nk
    one = pl.Buffered(1)

    def full(shape):
        return pl.BlockSpec(shape, lambda j: (0,) * len(shape), pipeline_mode=one)

    in_specs = [
        pl.BlockSpec((DP, 1, kt, Vp), lambda j: (0, j // nk, j % nk, 0)),
        full((1, V)),
        pl.BlockSpec((kt, 1), lambda j: (base + j, 0)),
        pl.BlockSpec((kt, FL), lambda j: (base + j, 0)),
        full((V, FL)), full((V, FL)), full((TS, V)),
    ]
    args = [eb, rs, gcol, W, dh, dl, sr]
    out_shape = [jax.ShapeDtypeStruct((D, FL), f32), jax.ShapeDtypeStruct((TS, D // 2), bf16)]
    out_specs = [pl.BlockSpec((kt, FL), lambda j: (base + j, 0)), pl.BlockSpec((TS, kt), lambda j: (0, j))]
    scratch = []
    alias = {}
    if last:
        N = ids.shape[0]
        in_specs += [full((FL, V)), full((N, 1)), pl.BlockSpec(memory_space=pl.ANY)]
        args += [up, ids, dw]
        alias = {9: 0}
        out_shape.append(jax.ShapeDtypeStruct((N, FL), bf16))
        out_specs.append(full((N, FL)))
        scratch = [pltpu.VMEM((FL, V), f32), pltpu.VMEM((FL, V), bf16)]
    else:
        out_shape.append(jax.ShapeDtypeStruct((FL, V), f32))
        out_specs.append(full((FL, V)))
    flops = 2 * V * FL * (D // 2) * 3 + (2 * V * V * FL if last else 0)
    return pl.pallas_call(
        functools.partial(forward_kernel, last, DP),
        grid=(C * nk,),
        in_specs=in_specs,
        out_specs=out_specs,
        out_shape=out_shape,
        scratch_shapes=scratch,
        input_output_aliases=alias,
        cost_estimate=pl.CostEstimate(flops=flops, bytes_accessed=30 << 20, transcendentals=0),
        compiler_params=pltpu.CompilerParams(dimension_semantics=("arbitrary",), vmem_limit_bytes=56 << 20),
        name="forward",
    )(*args)


barrier = lax.optimization_barrier


def split3(a):
    hi = lax.reduce_precision(a, 8, 7)
    mi = lax.reduce_precision(a - hi, 8, 7)
    lo = a - hi - mi
    return hi.astype(bf16), mi.astype(bf16), lo.astype(bf16)


def solution(mesh):
    G = mesh.shape['tp']
    DP = mesh.shape['dp']
    C = 2
    Z = G // C
    groups = [[d * G + z * C + c for d in range(DP) for c in range(C)] for z in range(Z)]

    def shift(k):
        return [(z * C + c, ((z + k) % Z) * C + c) for z in range(Z) for c in range(C)]

    swap = [(i, i ^ 1) for i in range(G)]

    def program(ids, E, g, W, du, dres):
        K, T = ids.shape
        N = K * T
        V, DL = E.shape
        D = g.shape[0]
        FL = W.shape[1]
        TL = T // G
        Vp = V // DP
        Dq = D // (2 * C)
        r = lax.axis_index('tp')
        grp = lax.axis_index('dp')
        z = r // C
        c = r % C
        gf = g.astype(f32)
        idf = ids.reshape(N)

        duf = du.reshape(N, FL)
        iota = jnp.arange(V, dtype=jnp.int32)

        Ep = lax.dynamic_slice_in_dim(E, grp * Vp, Vp, axis=0)
        AT = lax.all_gather(Ep.T, 'tp', axis=0, tiled=True)

        W4 = W.reshape(Z, C, DL, FL)
        Wm = lax.dynamic_index_in_dim(W4, c, 1, False)
        Ws = lax.dynamic_index_in_dim(W4, 1 - c, 1, False)
        du_o = lax.ppermute(duf, 'tp', swap)
        W_o = lax.ppermute(Ws, 'tp', swap)

        onehot = (iota[:, None] == idf[None, :]).astype(bf16)
        DU = jnp.dot(onehot, duf, preferred_element_type=f32)
        dh = lax.reduce_precision(DU, 8, 7)
        dl = (DU - dh).astype(bf16)
        dh = dh.astype(bf16)
        xl = jnp.take(E, idf, axis=0)
        dr4 = dres.reshape(K, TL, G, DL)
        du_o, W_o, dh, dl, xl = barrier((du_o, W_o, dh, dl, xl))

        duc = jnp.concatenate([duf, du_o], axis=1)
        Wc = jnp.concatenate([Wm, W_o], axis=2)
        H = N // 2
        F = Z // 2

        def part(dist):
            wz = lax.dynamic_index_in_dim(Wc, lax.rem(z + dist + Z, Z), 0, False)
            return jnp.einsum('tf,df->td', duc, wz, preferred_element_type=f32)

        streams = [(0, 1, F), (1, -1, F), (0, -1, F - 1), (1, 1, F - 1)]
        parts = {F: part(F)}
        parts[-F] = parts[F]
        for s in (-1, 1):
            parts[s * (F - 1)] = part(s * (F - 1))
        half = lambda a, h: lax.slice_in_dim(a, h * H, (h + 1) * H, axis=0)
        bufs = {st: half(parts[st[1] * st[2]], st[0]).astype(bf16) for st in streams}
        AT, dr4, _ = barrier((AT, dr4, tuple(bufs.values())))
        acc = {0: [], 1: []}

        def hop(bufs):
            out = {}
            for st, b in bufs.items():
                out[st] = lax.ppermute(b, 'tp', shift(st[1]))
            return out

        def add(moved, k, hook):
            nxt = {}
            for (h, s, L), b in moved.items():
                if k == L:
                    acc[h].append(b)
                else:
                    d = s * (L - k)
                    if d not in parts:
                        parts[d] = part(d)
                    p, _ = barrier((half(parts[d], h), hook))
                    nxt[(h, s, L)] = b.astype(f32) + p
            return nxt

        moved = hop(bufs)
        dc = lax.all_to_all(dr4, 'tp', 2, 0, tiled=False)
        dresc = dc.reshape(G, K, TL, DL).transpose(1, 0, 2, 3).reshape(N, DL)

        af = AT.astype(f32)
        ss = jnp.sum(af * af, axis=0, keepdims=True)
        rsp = lax.rsqrt(ss / D + EPS)
        pad = jnp.concatenate(list(split3(rsp)) + [jnp.zeros((5, Vp), bf16)], axis=0)
        b1 = jnp.concatenate([lax.dynamic_slice_in_dim(AT, c * Dq, Dq, axis=0), pad], axis=0)
        b2 = lax.dynamic_slice_in_dim(AT, D // 2 + c * Dq, Dq, axis=0)
        b1, b2 = barrier((b1, b2))
        e1 = lax.all_gather(b1, ('dp', 'tp'), axis_index_groups=groups, axis=0, tiled=False)
        e2 = lax.all_gather(b2, ('dp', 'tp'), axis_index_groups=groups, axis=0, tiled=False)
        e1 = e1.reshape(DP, C, Dq + 8, Vp)
        e2 = e2.reshape(DP, C, Dq, Vp)
        rp = e1[:, 0, Dq:Dq + 3, :].astype(f32)
        rs2 = (rp[:, 0] + rp[:, 1] + rp[:, 2]).reshape(1, V)

        idr = lax.dynamic_slice_in_dim(ids, r * TL, TL, axis=1).reshape(K * TL)
        sr = (idr[:, None] == iota[None, :]).astype(bf16)
        gcol = gf.reshape(D, 1)

        bufs = add(moved, 1, b2)
        gcol, _ = barrier((gcol, tuple(bufs.values())))
        moved = hop(bufs)
        dw1, x1, up = forward(0, e1, rs2, gcol, W, dh, dl, sr)
        bufs = add(moved, 2, x1)
        gcol, _ = barrier((gcol, tuple(bufs.values())))
        moved = hop(bufs)
        dW, x2, u = forward(1, e2, rs2, gcol, W, dh, dl, sr, up, idf.reshape(N, 1), dw1)
        for k in range(3, F + 1):
            bufs = add(moved, k, x2)
            moved = hop(bufs)
        parts[0] = part(0)
        dn = jnp.concatenate([half(parts[0], h) + sum(b.astype(f32) for b in acc[h]) for h in (0, 1)], axis=0)
        xo = jnp.concatenate([x1, x2], axis=1).reshape(K, TL, D)
        u = u.reshape(K, T, FL)

        rst = jnp.sum(jnp.where(idf[:, None] == iota[None, :], rs2, 0.0), axis=1)
        gl = lax.dynamic_slice_in_dim(gf, r * DL, DL)
        nh = xl.astype(f32) * rst[:, None]
        gdn = gl * dn
        sp = jnp.sum(nh * gdn, axis=1)
        dgl = jnp.sum(dn * nh, axis=0)
        small = exchange(G, jnp.concatenate([sp, dgl]).reshape((N + DL) // 128, 128)).reshape(G, N + DL)
        s = jnp.sum(small[:, :N], axis=0) / D
        dg = small[:, N:].reshape(D)
        dx = dresc.astype(f32) + rst[:, None] * (gdn - nh * s[:, None])
        d3 = jnp.dot(onehot, jnp.concatenate(split3(dx), axis=1), preferred_element_type=f32)
        dE = d3[:, :DL] + d3[:, DL:2 * DL] + d3[:, 2 * DL:]
        return u, xo, dE, dW, dg

    return jax.shard_map(
        program,
        mesh=mesh,
        in_specs=(P('dp', None), P(None, 'tp'), P(), P(None, 'tp'), P('dp', None, 'tp'), P('dp', 'tp', None)),
        out_specs=(P('dp', None, 'tp'), P('dp', 'tp', None), P('dp', 'tp'), P('dp', 'tp'), P('dp')),
        check_vma=False,
    )
```

```python
import functools

import jax
import jax.numpy as jnp
from jax import lax
from jax.experimental import pallas as pl
from jax.experimental.pallas import tpu as pltpu
from jax.sharding import PartitionSpec as P


EPS = 1e-6
MESH = pl.DeviceIdType.MESH
f32 = jnp.float32
bf16 = jnp.bfloat16


def step_kernel(nrecv, idx_ref, a_ref, b_ref, wa_ref, wb_ref, *refs):
    nt = (((1,), (1,)), ((), ()))
    o = lax.dot_general(a_ref[...], wa_ref[...], nt, preferred_element_type=f32)
    o += lax.dot_general(b_ref[...], wb_ref[...], nt, preferred_element_type=f32)
    for i in range(nrecv):
        o += refs[i][...].astype(f32)
    refs[nrecv][...] = o.astype(refs[nrecv].dtype)


def ring_step(h, idx, a, b, W, Wo, recvs, dtype):
    N, FL = a.shape
    DL = Wo.shape[1]
    M = N // 2
    bm = 512
    nb = M // bm
    row = lambda i, s: (h * nb + i, 0)
    out = lambda i, s: (i, 0)
    return pl.pallas_call(
        functools.partial(step_kernel, len(recvs)),
        grid_spec=pltpu.PrefetchScalarGridSpec(
            num_scalar_prefetch=1,
            grid=(nb,),
            in_specs=[
                pl.BlockSpec((bm, FL), row), pl.BlockSpec((bm, FL), row),
                pl.BlockSpec((DL, FL), lambda i, s: (s[0], 0)), pl.BlockSpec((DL, FL), lambda i, s: (s[1], 0)),
            ] + [pl.BlockSpec((bm, DL), out) for _ in recvs],
            out_specs=pl.BlockSpec((bm, DL), out),
        ),
        out_shape=jax.ShapeDtypeStruct((M, DL), dtype),
        cost_estimate=pl.CostEstimate(flops=4 * M * DL * FL, bytes_accessed=6 << 20, transcendentals=0),
        compiler_params=pltpu.CompilerParams(dimension_semantics=("arbitrary",), vmem_limit_bytes=16 << 20),
        name="ring_step",
    )(idx, a, b, W, Wo.reshape(-1, FL), *recvs)


def tail_kernel(G, s_ref, ids_ref, q_ref, o_ref, d_ref, send, recv):
    me = lax.axis_index('tp')
    bar = pltpu.get_barrier_semaphore()
    for k in range(1, G):
        pl.semaphore_signal(bar, inc=1, device_id={'tp': lax.rem(me + k, G)}, device_id_type=MESH)
    pl.semaphore_wait(bar, G - 1)
    copies = []
    for k in range(1, G):
        cp = pltpu.make_async_remote_copy(
            src_ref=s_ref, dst_ref=o_ref.at[me], send_sem=send.at[k - 1], recv_sem=recv.at[k - 1],
            device_id={'tp': lax.rem(me + k, G)}, device_id_type=MESH)
        cp.start()
        copies.append(cp)
    o_ref[me] = s_ref[...]
    N, Q = q_ref.shape
    DL = Q // 3
    vb = 512

    def block(i, carry):
        rows = pl.ds(pl.multiple_of(i * vb, vb), vb)
        hot = lax.broadcasted_iota(jnp.int32, (vb, N), 0) + i * vb == ids_ref[...]
        d3 = jnp.dot(jnp.where(hot, 1.0, 0.0).astype(bf16), q_ref[...], preferred_element_type=f32)
        d_ref[rows, :] = d3[:, :DL] + d3[:, DL:2 * DL] + d3[:, 2 * DL:]
        return carry

    lax.fori_loop(0, d_ref.shape[0] // vb, block, 0)
    for cp in copies:
        cp.wait()


def tail(G, V, small, ids, q):
    vm = pl.BlockSpec(memory_space=pltpu.VMEM)
    return pl.pallas_call(
        functools.partial(tail_kernel, G),
        out_shape=(jax.ShapeDtypeStruct((G,) + small.shape, f32), jax.ShapeDtypeStruct((V, q.shape[1] // 3), f32)),
        in_specs=[vm, vm, vm],
        out_specs=(vm, vm),
        scratch_shapes=[pltpu.SemaphoreType.DMA((G - 1,)), pltpu.SemaphoreType.DMA((G - 1,))],
        cost_estimate=pl.CostEstimate(flops=2 * V * q.shape[0] * q.shape[1], bytes_accessed=6 << 20, transcendentals=0),
        compiler_params=pltpu.CompilerParams(collective_id=0, has_side_effects=True, vmem_limit_bytes=40 << 20),
        name="tail",
    )(small, ids, q)


def forward_kernel(last, DP, *refs):
    if last:
        (eb_ref, rs_ref, g_ref, w_ref, dh_ref, dl_ref, sr_ref, up_ref, ids_ref, _,
         dw_ref, xo_ref, u_ref, acc_ref, ub_ref) = refs
    else:
        (eb_ref, rs_ref, g_ref, w_ref, dh_ref, dl_ref, sr_ref, dw_ref, xo_ref, acc_ref) = refs
    j = pl.program_id(0)
    x = jnp.concatenate([eb_ref[i, 0] for i in range(DP)], axis=1)
    n = (x.astype(f32) * rs_ref[...] * g_ref[...]).astype(bf16)
    dw_ref[...] = (jnp.dot(n, dh_ref[...], preferred_element_type=f32)
                   + jnp.dot(n, dl_ref[...], preferred_element_type=f32))
    xo_ref[...] = lax.dot_general(sr_ref[...], x, (((1,), (1,)), ((), ())),
                                  preferred_element_type=f32).astype(bf16)
    up = lax.dot_general(w_ref[...], n, (((0,), (0,)), ((), ())), preferred_element_type=f32)

    @pl.when(j == 0)
    def _():
        acc_ref[...] = up + up_ref[...] if last else up

    @pl.when(j > 0)
    def _():
        acc_ref[...] += up

    if last:
        @pl.when(j == pl.num_programs(0) - 1)
        def _():
            ub_ref[...] = acc_ref[...].astype(bf16)
            tb = 512

            def step(i, carry):
                rows = pl.ds(pl.multiple_of(i * tb, tb), tb)
                V = ub_ref.shape[1]
                hot = lax.broadcasted_iota(jnp.int32, (tb, V), 1) == ids_ref[rows, :]
                s = jnp.where(hot, 1.0, 0.0).astype(bf16)
                u_ref[rows, :] = lax.dot_general(s, ub_ref[...], (((1,), (1,)), ((), ())),
                                                 preferred_element_type=f32).astype(bf16)
                return carry

            lax.fori_loop(0, u_ref.shape[0] // tb, step, 0)


def forward(q, eb, rs, gcol, W, dh, dl, sr, up=None, ids=None, dw=None):
    last = q == 1
    DP, C, _, Vp = eb.shape
    V = DP * Vp
    D, FL = W.shape
    Dq = D // (2 * C)
    kt = 512
    nk = Dq // kt
    TS = sr.shape[0]
    base = q * C * nk
    one = pl.Buffered(1)

    def full(shape):
        return pl.BlockSpec(shape, lambda j: (0,) * len(shape), pipeline_mode=one)

    in_specs = [
        pl.BlockSpec((DP, 1, kt, Vp), lambda j: (0, j // nk, j % nk, 0)),
        full((1, V)),
        pl.BlockSpec((kt, 1), lambda j: (base + j, 0)),
        pl.BlockSpec((kt, FL), lambda j: (base + j, 0)),
        full((V, FL)), full((V, FL)), full((TS, V)),
    ]
    args = [eb, rs, gcol, W, dh, dl, sr]
    out_shape = [jax.ShapeDtypeStruct((D, FL), f32), jax.ShapeDtypeStruct((TS, D // 2), bf16)]
    out_specs = [pl.BlockSpec((kt, FL), lambda j: (base + j, 0)), pl.BlockSpec((TS, kt), lambda j: (0, j))]
    scratch = []
    alias = {}
    if last:
        N = ids.shape[0]
        in_specs += [full((FL, V)), full((N, 1)), pl.BlockSpec(memory_space=pl.ANY)]
        args += [up, ids, dw]
        alias = {9: 0}
        out_shape.append(jax.ShapeDtypeStruct((N, FL), bf16))
        out_specs.append(full((N, FL)))
        scratch = [pltpu.VMEM((FL, V), f32), pltpu.VMEM((FL, V), bf16)]
    else:
        out_shape.append(jax.ShapeDtypeStruct((FL, V), f32))
        out_specs.append(full((FL, V)))
    flops = 2 * V * FL * (D // 2) * 3 + (2 * V * V * FL if last else 0)
    return pl.pallas_call(
        functools.partial(forward_kernel, last, DP),
        grid=(C * nk,),
        in_specs=in_specs,
        out_specs=out_specs,
        out_shape=out_shape,
        scratch_shapes=scratch,
        input_output_aliases=alias,
        cost_estimate=pl.CostEstimate(flops=flops, bytes_accessed=30 << 20, transcendentals=0),
        compiler_params=pltpu.CompilerParams(dimension_semantics=("arbitrary",), vmem_limit_bytes=56 << 20),
        name="forward",
    )(*args)


barrier = lax.optimization_barrier


def split3(a):
    hi = lax.reduce_precision(a, 8, 7)
    mi = lax.reduce_precision(a - hi, 8, 7)
    lo = a - hi - mi
    return hi.astype(bf16), mi.astype(bf16), lo.astype(bf16)


def solution(mesh):
    G = mesh.shape['tp']
    DP = mesh.shape['dp']
    C = 2
    Z = G // C
    groups = [[d * G + z * C + c for d in range(DP) for c in range(C)] for z in range(Z)]

    def shift(k):
        return [(z * C + c, ((z + k) % Z) * C + c) for z in range(Z) for c in range(C)]

    swap = [(i, i ^ 1) for i in range(G)]

    def program(ids, E, g, W, du, dres):
        K, T = ids.shape
        N = K * T
        V, DL = E.shape
        D = g.shape[0]
        FL = W.shape[1]
        TL = T // G
        Vp = V // DP
        Dq = D // (2 * C)
        r = lax.axis_index('tp')
        grp = lax.axis_index('dp')
        z = r // C
        c = r % C
        gf = g.astype(f32)
        idf = ids.reshape(N)

        duf = du.reshape(N, FL)
        iota = jnp.arange(V, dtype=jnp.int32)

        Ep = lax.dynamic_slice_in_dim(E, grp * Vp, Vp, axis=0)
        AT = lax.all_gather(Ep.T, 'tp', axis=0, tiled=True)

        du_o = lax.ppermute(duf, 'tp', swap)
        Ws = lax.dynamic_index_in_dim(W.reshape(Z, C, DL, FL), 1 - c, 1, False)
        W_o = lax.ppermute(Ws, 'tp', swap)
        dc = lax.all_to_all(dres.reshape(K, TL, G, DL), 'tp', 2, 0, tiled=False)
        dresc = dc.reshape(G, K, TL, DL).transpose(1, 0, 2, 3).reshape(N, DL)
        gcol = gf.reshape(D, 1)
        du_o, W_o, gcol = barrier((du_o, W_o, gcol))
        F = Z // 2

        def part(h, dist, recvs, dtype):
            zd = lax.rem(z + dist + Z, Z)
            idx = jnp.stack([zd * C + c, zd])
            return ring_step(h, idx, duf, du_o, W, W_o, recvs, dtype)

        streams = [(0, 1, F), (1, -1, F), (1, 1, F - 1), (0, -1, F - 1)]
        acc = {0: [], 1: []}

        def hop(bufs):
            out = {}
            for st, b in bufs.items():
                out[st] = lax.ppermute(b, 'tp', shift(st[1]))
            return out

        def add(moved, k, hook):
            nxt = {}
            for (h, s, L), b in moved.items():
                if k == L:
                    acc[h].append(b)
                else:
                    b, _ = barrier((b, hook))
                    nxt[(h, s, L)] = part(h, s * (L - k), [b], f32)
            return nxt

        bufs = {(h, s, L): part(h, s * L, [], bf16) for h, s, L in streams}
        idh, _ = barrier((idf, tuple(bufs.values())))
        moved = hop(bufs)

        onehot = (iota[:, None] == idh[None, :]).astype(bf16)
        DU = jnp.dot(onehot, duf, preferred_element_type=f32)
        dh = lax.reduce_precision(DU, 8, 7)
        dl = (DU - dh).astype(bf16)
        dh = dh.astype(bf16)

        af = AT.astype(f32)
        ss = jnp.sum(af * af, axis=0, keepdims=True)
        rsp = lax.rsqrt(ss / D + EPS)
        pad = jnp.concatenate(list(split3(rsp)) + [jnp.zeros((5, Vp), bf16)], axis=0)
        b1 = jnp.concatenate([lax.dynamic_slice_in_dim(AT, c * Dq, Dq, axis=0), pad], axis=0)
        b2 = lax.dynamic_slice_in_dim(AT, D // 2 + c * Dq, Dq, axis=0)
        b1, b2 = barrier((b1, b2))
        e1 = lax.all_gather(b1, ('dp', 'tp'), axis_index_groups=groups, axis=0, tiled=False)
        e2 = lax.all_gather(b2, ('dp', 'tp'), axis_index_groups=groups, axis=0, tiled=False)
        e1 = e1.reshape(DP, C, Dq + 8, Vp)
        e2 = e2.reshape(DP, C, Dq, Vp)
        rp = e1[:, 0, Dq:Dq + 3, :].astype(f32)
        rs2 = (rp[:, 0] + rp[:, 1] + rp[:, 2]).reshape(1, V)

        bufs = add(moved, 1, b2)
        idx, _ = barrier((idf, tuple(bufs.values())))
        moved = hop(bufs)
        xl = jnp.take(E, idx, axis=0)
        idr = lax.dynamic_slice_in_dim(ids, r * TL, TL, axis=1).reshape(K * TL)
        sr = (idr[:, None] == iota[None, :]).astype(bf16)
        idc = idx.reshape(N, 1)
        rs2, sr, idc, xl, _ = barrier((rs2, sr, idc, xl, dresc))
        dw1, x1, up = forward(0, e1, rs2, gcol, W, dh, dl, sr)
        bufs = add(moved, 2, x1)
        rs2, _ = barrier((rs2, tuple(bufs.values())))
        moved = hop(bufs)
        rst = jnp.sum(jnp.where(idx[:, None] == iota[None, :], rs2, 0.0), axis=1)
        for k in range(3, F):
            bufs = add(moved, k, rst)
            rs2, _ = barrier((rs2, tuple(bufs.values())))
            moved = hop(bufs)
        dW, x2, u = forward(1, e2, rs2, gcol, W, dh, dl, sr, up, idc, dw1)
        moved = {st: barrier((b, x2))[0] for st, b in moved.items()}
        add(moved, F, x2)
        dn = jnp.concatenate([part(h, 0, acc[h], f32) for h in (0, 1)], axis=0)
        xo = jnp.concatenate([x1, x2], axis=1).reshape(K, TL, D)
        u = u.reshape(K, T, FL)

        gl = lax.dynamic_slice_in_dim(gf, r * DL, DL)
        nh = xl.astype(f32) * rst[:, None]
        gdn = gl * dn
        sp = jnp.sum(nh * gdn, axis=1)
        dgl = jnp.sum(dn * nh, axis=0)
        small = jnp.concatenate([sp, dgl]).reshape((N + DL) // 128, 128)
        q = jnp.concatenate(split3(dresc.astype(f32) + rst[:, None] * gdn), axis=1)
        small, dA = tail(G, V, small, idx.reshape(1, N), q)
        small = small.reshape(G, N + DL)
        s = jnp.sum(small[:, :N], axis=0) / D
        dg = small[:, N:].reshape(D)
        sv = jnp.sum(jnp.where(iota[:, None] == idf[None, :], s[None, :], 0.0), axis=1)
        rv = rs2.reshape(V, 1)
        dE = dA - rv * (E.astype(f32) * rv) * sv[:, None]
        return u, xo, dE, dW, dg

    return jax.shard_map(
        program,
        mesh=mesh,
        in_specs=(P('dp', None), P(None, 'tp'), P(), P(None, 'tp'), P('dp', None, 'tp'), P('dp', 'tp', None)),
        out_specs=(P('dp', None, 'tp'), P('dp', 'tp', None), P('dp', 'tp'), P('dp', 'tp'), P('dp')),
        check_vma=False,
    )
```

```python
import functools

import jax
import jax.numpy as jnp
from jax import lax
from jax.experimental import pallas as pl
from jax.experimental.layout import Layout, with_layout_constraint
from jax.experimental.pallas import tpu as pltpu
from jax.sharding import PartitionSpec as P


EPS = 1e-6
MESH = pl.DeviceIdType.MESH
f32 = jnp.float32
bf16 = jnp.bfloat16


def send_all(G, s_ref, o_ref, send, recv):
    me = lax.axis_index('tp')
    bar = pltpu.get_barrier_semaphore()
    for k in range(1, G):
        pl.semaphore_signal(bar, inc=1, device_id={'tp': lax.rem(me + k, G)}, device_id_type=MESH)
    pl.semaphore_wait(bar, G - 1)
    copies = []
    for k in range(1, G):
        cp = pltpu.make_async_remote_copy(
            src_ref=s_ref, dst_ref=o_ref.at[me], send_sem=send.at[k - 1], recv_sem=recv.at[k - 1],
            device_id={'tp': lax.rem(me + k, G)}, device_id_type=MESH)
        cp.start()
        copies.append(cp)
    o_ref[me] = s_ref[...]
    return copies


def exchange_kernel(G, s_ref, o_ref, send, recv):
    for cp in send_all(G, s_ref, o_ref, send, recv):
        cp.wait()


def exchange(G, small):
    vm = pl.BlockSpec(memory_space=pltpu.VMEM)
    return pl.pallas_call(
        functools.partial(exchange_kernel, G),
        out_shape=jax.ShapeDtypeStruct((G,) + small.shape, f32),
        in_specs=[vm],
        out_specs=vm,
        scratch_shapes=[pltpu.SemaphoreType.DMA((G - 1,)), pltpu.SemaphoreType.DMA((G - 1,))],
        cost_estimate=pl.CostEstimate(flops=1 << 30, bytes_accessed=1 << 20, transcendentals=0),
        compiler_params=pltpu.CompilerParams(collective_id=1, has_side_effects=True, vmem_limit_bytes=4 << 20),
        name="exchange",
    )(small)


def tail_kernel(G, s_ref, ids_ref, q_ref, o_ref, d_ref, send, recv):
    copies = send_all(G, s_ref, o_ref, send, recv)
    N, Q = q_ref.shape
    DL = Q // 3
    vb = 512

    def block(i, carry):
        rows = pl.ds(pl.multiple_of(i * vb, vb), vb)
        hot = lax.broadcasted_iota(jnp.int32, (vb, N), 0) + i * vb == ids_ref[...]
        d3 = jnp.dot(jnp.where(hot, 1.0, 0.0).astype(bf16), q_ref[...], preferred_element_type=f32)
        d_ref[rows, :] = d3[:, :DL] + d3[:, DL:2 * DL] + d3[:, 2 * DL:]
        return carry

    lax.fori_loop(0, d_ref.shape[0] // vb, block, 0)
    for cp in copies:
        cp.wait()


def tail(G, V, small, ids, q):
    vm = pl.BlockSpec(memory_space=pltpu.VMEM)
    return pl.pallas_call(
        functools.partial(tail_kernel, G),
        out_shape=(jax.ShapeDtypeStruct((G,) + small.shape, f32), jax.ShapeDtypeStruct((V, q.shape[1] // 3), f32)),
        in_specs=[vm, vm, vm],
        out_specs=(vm, vm),
        scratch_shapes=[pltpu.SemaphoreType.DMA((G - 1,)), pltpu.SemaphoreType.DMA((G - 1,))],
        cost_estimate=pl.CostEstimate(flops=2 * V * q.shape[0] * q.shape[1], bytes_accessed=6 << 20, transcendentals=0),
        compiler_params=pltpu.CompilerParams(collective_id=0, has_side_effects=True, vmem_limit_bytes=40 << 20),
        name="tail",
    )(small, ids, q)


def forward_kernel(last, DP, *refs):
    if last:
        (eb_ref, rs_ref, g_ref, w_ref, dh_ref, dl_ref, sr_ref, up_ref, ids_ref, _,
         dw_ref, xo_ref, u_ref, acc_ref, ub_ref) = refs
    else:
        (eb_ref, rs_ref, g_ref, w_ref, dh_ref, dl_ref, sr_ref, dw_ref, xo_ref, acc_ref) = refs
    j = pl.program_id(0)
    x = jnp.concatenate([eb_ref[i, 0] for i in range(DP)], axis=1)
    n = (x.astype(f32) * rs_ref[...] * g_ref[...]).astype(bf16)
    dw_ref[...] = (jnp.dot(n, dh_ref[...], preferred_element_type=f32)
                   + jnp.dot(n, dl_ref[...], preferred_element_type=f32))
    xo_ref[...] = lax.dot_general(sr_ref[...], x, (((1,), (1,)), ((), ())),
                                  preferred_element_type=f32).astype(bf16)
    up = lax.dot_general(w_ref[...], n, (((0,), (0,)), ((), ())), preferred_element_type=f32)

    @pl.when(j == 0)
    def _():
        acc_ref[...] = up + up_ref[...] if last else up

    @pl.when(j > 0)
    def _():
        acc_ref[...] += up

    if last:
        @pl.when(j == pl.num_programs(0) - 1)
        def _():
            ub_ref[...] = acc_ref[...].astype(bf16)
            tb = 512

            def step(i, carry):
                rows = pl.ds(pl.multiple_of(i * tb, tb), tb)
                V = ub_ref.shape[1]
                hot = lax.broadcasted_iota(jnp.int32, (tb, V), 1) == ids_ref[rows, :]
                s = jnp.where(hot, 1.0, 0.0).astype(bf16)
                u_ref[rows, :] = lax.dot_general(s, ub_ref[...], (((1,), (1,)), ((), ())),
                                                 preferred_element_type=f32).astype(bf16)
                return carry

            lax.fori_loop(0, u_ref.shape[0] // tb, step, 0)


def forward(q, eb, rs, gcol, W, dh, dl, sr, up=None, ids=None, dw=None):
    last = q == 1
    DP, C, _, Vp = eb.shape
    V = DP * Vp
    D, FL = W.shape
    Dq = D // (2 * C)
    kt = 512
    nk = Dq // kt
    TS = sr.shape[0]
    base = q * C * nk
    one = pl.Buffered(1)

    def full(shape):
        return pl.BlockSpec(shape, lambda j: (0,) * len(shape), pipeline_mode=one)

    in_specs = [
        pl.BlockSpec((DP, 1, kt, Vp), lambda j: (0, j // nk, j % nk, 0)),
        full((1, V)),
        pl.BlockSpec((kt, 1), lambda j: (base + j, 0)),
        pl.BlockSpec((kt, FL), lambda j: (base + j, 0)),
        full((V, FL)), full((V, FL)), full((TS, V)),
    ]
    args = [eb, rs, gcol, W, dh, dl, sr]
    out_shape = [jax.ShapeDtypeStruct((D, FL), f32), jax.ShapeDtypeStruct((TS, D // 2), bf16)]
    out_specs = [pl.BlockSpec((kt, FL), lambda j: (base + j, 0)), pl.BlockSpec((TS, kt), lambda j: (0, j))]
    scratch = []
    alias = {}
    if last:
        N = ids.shape[0]
        in_specs += [full((FL, V)), full((N, 1)), pl.BlockSpec(memory_space=pl.ANY)]
        args += [up, ids, dw]
        alias = {9: 0}
        out_shape.append(jax.ShapeDtypeStruct((N, FL), bf16))
        out_specs.append(full((N, FL)))
        scratch = [pltpu.VMEM((FL, V), f32), pltpu.VMEM((FL, V), bf16)]
    else:
        out_shape.append(jax.ShapeDtypeStruct((FL, V), f32))
        out_specs.append(full((FL, V)))
    flops = 2 * V * FL * (D // 2) * 3 + (2 * V * V * FL if last else 0)
    return pl.pallas_call(
        functools.partial(forward_kernel, last, DP),
        grid=(C * nk,),
        in_specs=in_specs,
        out_specs=out_specs,
        out_shape=out_shape,
        scratch_shapes=scratch,
        input_output_aliases=alias,
        cost_estimate=pl.CostEstimate(flops=flops, bytes_accessed=30 << 20, transcendentals=0),
        compiler_params=pltpu.CompilerParams(dimension_semantics=("arbitrary",), vmem_limit_bytes=(52 if last else 40) << 20),
        name="forward",
    )(*args)


barrier = lax.optimization_barrier


def rows(a):
    return with_layout_constraint(a, Layout(major_to_minor=(0, 1)))


def split3(a):
    hi = lax.reduce_precision(a, 8, 7)
    mi = lax.reduce_precision(a - hi, 8, 7)
    lo = a - hi - mi
    return hi.astype(bf16), mi.astype(bf16), lo.astype(bf16)


def solution(mesh):
    G = mesh.shape['tp']
    DP = mesh.shape['dp']
    C = 2
    Z = G // C
    groups = [[d * G + z * C + c for d in range(DP) for c in range(C)] for z in range(Z)]

    def shift(k):
        return [(z * C + c, ((z + k) % Z) * C + c) for z in range(Z) for c in range(C)]

    swap = [(i, i ^ 1) for i in range(G)]

    def program(ids, E, g, W, du, dres):
        K, T = ids.shape
        N = K * T
        V, DL = E.shape
        D = g.shape[0]
        FL = W.shape[1]
        TL = T // G
        Vp = V // DP
        Dq = D // (2 * C)
        r = lax.axis_index('tp')
        grp = lax.axis_index('dp')
        z = r // C
        c = r % C
        gf = g.astype(f32)
        idf = ids.reshape(N)

        duf = du.reshape(N, FL)
        iota = jnp.arange(V, dtype=jnp.int32)

        Ep = lax.dynamic_slice_in_dim(E, grp * Vp, Vp, axis=0)
        AT = lax.all_gather(rows(Ep.T), 'tp', axis=0, tiled=True)

        du_o = lax.ppermute(duf, 'tp', swap)
        Ws = lax.dynamic_index_in_dim(W.reshape(Z, C, DL, FL), 1 - c, 1, False)
        W_o = lax.ppermute(Ws, 'tp', swap)
        el = E.astype(f32)
        ssl = jnp.sum(el * el, axis=1)
        ssl, _ = barrier((ssl, Ws))
        ssg = exchange(G, ssl.reshape(V // 128, 128))
        rs2 = lax.rsqrt(jnp.sum(ssg, axis=0) / D + EPS).reshape(1, V)
        rst = jnp.sum(jnp.where(idf[:, None] == iota[None, :], rs2, 0.0), axis=1)
        gcol = gf.reshape(D, 1)
        du_o, W_o, gcol, rs2 = barrier((du_o, W_o, gcol, rs2))
        H = N // 2
        F = Z // 2
        half = lambda a, h: lax.slice_in_dim(a, h * H, (h + 1) * H, axis=0)
        duc = jnp.concatenate([duf, du_o], axis=1)

        def part(dist, Wo):
            zd = lax.rem(z + dist + Z, Z)
            own = lax.dynamic_slice_in_dim(W, (zd * C + c) * DL, DL, axis=0)
            wz = jnp.concatenate([own, lax.dynamic_index_in_dim(Wo, zd, 0, False)], axis=1)
            return jnp.einsum('tf,df->td', duc, wz, preferred_element_type=f32)

        streams = [(0, 1, F), (1, -1, F), (1, 1, F - 1), (0, -1, F - 1)]
        acc = {0: [], 1: []}

        def hop(bufs):
            out = {}
            for st, b in bufs.items():
                out[st] = lax.ppermute(b, 'tp', shift(st[1]))
            return out

        def add(moved, k, hook):
            nxt = {}
            for (h, s, L), b in moved.items():
                if k == L:
                    acc[h].append(b)
                else:
                    p, b, _ = barrier((parts[s * (L - k)], b, hook))
                    nxt[(h, s, L)] = b.astype(f32) + half(p, h)
            return nxt

        parts = {F: part(F, W_o)}
        parts[-F] = parts[F]
        for d in (F - 1, 1 - F):
            parts[d] = part(d, W_o)
        bufs = {(h, s, L): half(parts[s * L], h).astype(bf16) for h, s, L in streams}
        idh, _ = barrier((idf, tuple(bufs.values())))
        moved = hop(bufs)

        onehot = (iota[:, None] == idh[None, :]).astype(bf16)
        DU = jnp.dot(onehot, duf, preferred_element_type=f32)
        dh = lax.reduce_precision(DU, 8, 7)
        dl = (DU - dh).astype(bf16)
        dh = dh.astype(bf16)

        b1 = lax.dynamic_slice_in_dim(AT, c * Dq, Dq, axis=0)
        b2 = lax.dynamic_slice_in_dim(AT, D // 2 + c * Dq, Dq, axis=0)
        b1, b2 = barrier((rows(b1), rows(b2)))
        e1 = lax.all_gather(b1, ('dp', 'tp'), axis_index_groups=groups, axis=0, tiled=False).reshape(DP, C, Dq, Vp)
        e2 = lax.all_gather(b2, ('dp', 'tp'), axis_index_groups=groups, axis=0, tiled=False).reshape(DP, C, Dq, Vp)
        Wo2, _ = barrier((W_o, b2))
        for d in range(F - 2, 0, -1):
            for s in (1, -1):
                parts[s * d] = part(s * d, Wo2)
        parts[0] = part(0, Wo2)

        bufs = add(moved, 1, b2)
        idx, _ = barrier((idf, tuple(bufs.values())))
        moved = hop(bufs)
        drs, idx = barrier((dres, idx))
        dc = lax.all_to_all(drs.reshape(K, TL, G, DL), 'tp', 2, 0, tiled=False)
        dresc = dc.reshape(G, K, TL, DL).transpose(1, 0, 2, 3).reshape(N, DL)
        xl = jnp.take(E, idx, axis=0)
        idr = lax.dynamic_slice_in_dim(ids, r * TL, TL, axis=1).reshape(K * TL)
        sr = (idr[:, None] == iota[None, :]).astype(bf16)
        idc = idx.reshape(N, 1)
        rs2, sr, idc, xl = barrier((rs2, sr, idc, xl))
        dw1, x1, up = forward(0, e1, rs2, gcol, W, dh, dl, sr)
        bufs = add(moved, 2, x1)
        rs2, _ = barrier((rs2, tuple(bufs.values())))
        moved = hop(bufs)
        for k in range(3, F):
            bufs = add(moved, k, x1)
            rs2, _ = barrier((rs2, tuple(bufs.values())))
            moved = hop(bufs)
        dW, x2, u = forward(1, e2, rs2, gcol, W, dh, dl, sr, up, idc, dw1)
        moved = {st: barrier((b, x2))[0] for st, b in moved.items()}
        add(moved, F, x2)
        dn = jnp.concatenate([half(parts[0], h) + sum(b.astype(f32) for b in acc[h]) for h in (0, 1)], axis=0)
        xo = jnp.concatenate([x1, x2], axis=1).reshape(K, TL, D)
        u = u.reshape(K, T, FL)

        gl = lax.dynamic_slice_in_dim(gf, r * DL, DL)
        nh = xl.astype(f32) * rst[:, None]
        gdn = gl * dn
        sp = jnp.sum(nh * gdn, axis=1)
        dgl = jnp.sum(dn * nh, axis=0)
        small = jnp.concatenate([sp, dgl]).reshape((N + DL) // 128, 128)
        q = jnp.concatenate(split3(dresc.astype(f32) + rst[:, None] * gdn), axis=1)
        small, dA = tail(G, V, small, idx.reshape(1, N), q)
        small = small.reshape(G, N + DL)
        s = jnp.sum(small[:, :N], axis=0) / D
        dg = small[:, N:].reshape(D)
        sv = jnp.sum(jnp.where(iota[:, None] == idf[None, :], s[None, :], 0.0), axis=1)
        rv = rs2.reshape(V, 1)
        dE = dA - rv * (E.astype(f32) * rv) * sv[:, None]
        return u, xo, dE, dW, dg

    return jax.shard_map(
        program,
        mesh=mesh,
        in_specs=(P('dp', None), P(None, 'tp'), P(), P(None, 'tp'), P('dp', None, 'tp'), P('dp', 'tp', None)),
        out_specs=(P('dp', None, 'tp'), P('dp', 'tp', None), P('dp', 'tp'), P('dp', 'tp'), P('dp')),
        check_vma=False,
    )
```

```python
import functools

import jax
import jax.numpy as jnp
from jax import lax
from jax.experimental import pallas as pl
from jax.experimental.layout import Layout, with_layout_constraint
from jax.experimental.pallas import tpu as pltpu
from jax.sharding import PartitionSpec as P


EPS = 1e-6
MESH = pl.DeviceIdType.MESH
f32 = jnp.float32
bf16 = jnp.bfloat16


def parts_kernel(nb, idx_ref, a_ref, b_ref, wa_ref, wb_ref, *outs):
    nt = (((1,), (1,)), ((), ()))
    o = (lax.dot_general(a_ref[...], wa_ref[...], nt, preferred_element_type=f32)
         + lax.dot_general(b_ref[...], wb_ref[...], nt, preferred_element_type=f32)).astype(outs[0].dtype)
    for i in range(nb):
        @pl.when(pl.program_id(0) == i)
        def _(i=i):
            outs[i][...] = o


def chip_parts(blocks, z, c, Z, C, a, b, W, Wo, dtype):
    blocks = sorted(blocks, key=lambda t: t[1])
    nb = len(blocks)
    N, FL = a.shape
    DL = Wo.shape[1]
    M = N // 2
    zd = [lax.rem(z + d + Z, Z) for d, _ in blocks]
    idx = jnp.stack([q * C + c for q in zd] + zd)
    first = sum(1 for _, h in blocks if h == 0)
    row = lambda i, s: (jnp.where(i >= first, 1, 0), 0)
    outs = pl.pallas_call(
        functools.partial(parts_kernel, nb),
        grid_spec=pltpu.PrefetchScalarGridSpec(
            num_scalar_prefetch=1,
            grid=(nb,),
            in_specs=[
                pl.BlockSpec((M, FL), row), pl.BlockSpec((M, FL), row),
                pl.BlockSpec((DL, FL), lambda i, s: (s[i], 0)), pl.BlockSpec((DL, FL), lambda i, s: (s[nb + i], 0)),
            ],
            out_specs=[pl.BlockSpec((M, DL), lambda i, s: (0, 0)) for _ in blocks],
        ),
        out_shape=[jax.ShapeDtypeStruct((M, DL), dtype) for _ in blocks],
        cost_estimate=pl.CostEstimate(flops=4 * M * DL * FL * nb, bytes_accessed=8 << 20, transcendentals=0),
        compiler_params=pltpu.CompilerParams(dimension_semantics=("arbitrary",), vmem_limit_bytes=40 << 20),
        name="chip_parts",
    )(idx, a, b, W, Wo.reshape(-1, FL))
    return dict(zip(blocks, outs))


def rowsum_kernel(ids_ref, du_ref, e_ref, hi_ref, lo_ref, x_ref, acc_ref):
    i = pl.program_id(0)
    vb = e_ref.shape[0]
    hot = lax.broadcasted_iota(jnp.int32, (vb, du_ref.shape[0]), 0) + i * vb == ids_ref[...]
    hot = jnp.where(hot, 1.0, 0.0).astype(bf16)
    d = jnp.dot(hot, du_ref[...], preferred_element_type=f32)
    hi = d.astype(bf16)
    hi_ref[...] = hi
    lo_ref[...] = (d - hi.astype(f32)).astype(bf16)
    x = lax.dot_general(hot, e_ref[...], (((0,), (0,)), ((), ())), preferred_element_type=f32)

    @pl.when(i == 0)
    def _():
        acc_ref[...] = x

    @pl.when(i > 0)
    def _():
        acc_ref[...] += x

    @pl.when(i == pl.num_programs(0) - 1)
    def _():
        x_ref[...] = acc_ref[...].astype(bf16)


def rowsums(ids, du, E):
    N, FL = du.shape
    V, DL = E.shape
    vb = 512
    one = pl.Buffered(1)
    return pl.pallas_call(
        rowsum_kernel,
        grid=(V // vb,),
        in_specs=[
            pl.BlockSpec((1, N), lambda i: (0, 0)),
            pl.BlockSpec((N, FL), lambda i: (0, 0), pipeline_mode=one),
            pl.BlockSpec((vb, DL), lambda i: (i, 0)),
        ],
        out_specs=[pl.BlockSpec((vb, FL), lambda i: (i, 0)), pl.BlockSpec((vb, FL), lambda i: (i, 0)),
                   pl.BlockSpec((N, DL), lambda i: (0, 0))],
        out_shape=[jax.ShapeDtypeStruct((V, FL), bf16), jax.ShapeDtypeStruct((V, FL), bf16),
                   jax.ShapeDtypeStruct((N, DL), bf16)],
        scratch_shapes=[pltpu.VMEM((N, DL), f32)],
        cost_estimate=pl.CostEstimate(flops=2 * V * N * (FL + DL), bytes_accessed=12 << 20, transcendentals=0),
        compiler_params=pltpu.CompilerParams(dimension_semantics=("arbitrary",), vmem_limit_bytes=40 << 20),
        name="rowsums",
    )(ids, du, E)


def send_all(G, s_ref, o_ref, send, recv):
    me = lax.axis_index('tp')
    bar = pltpu.get_barrier_semaphore()
    for k in range(1, G):
        pl.semaphore_signal(bar, inc=1, device_id={'tp': lax.rem(me + k, G)}, device_id_type=MESH)
    pl.semaphore_wait(bar, G - 1)
    copies = []
    for k in range(1, G):
        cp = pltpu.make_async_remote_copy(
            src_ref=s_ref, dst_ref=o_ref.at[me], send_sem=send.at[k - 1], recv_sem=recv.at[k - 1],
            device_id={'tp': lax.rem(me + k, G)}, device_id_type=MESH)
        cp.start()
        copies.append(cp)
    o_ref[me] = s_ref[...]
    return copies


def exchange_kernel(G, s_ref, o_ref, send, recv):
    for cp in send_all(G, s_ref, o_ref, send, recv):
        cp.wait()


def exchange(G, small):
    vm = pl.BlockSpec(memory_space=pltpu.VMEM)
    return pl.pallas_call(
        functools.partial(exchange_kernel, G),
        out_shape=jax.ShapeDtypeStruct((G,) + small.shape, f32),
        in_specs=[vm],
        out_specs=vm,
        scratch_shapes=[pltpu.SemaphoreType.DMA((G - 1,)), pltpu.SemaphoreType.DMA((G - 1,))],
        cost_estimate=pl.CostEstimate(flops=1 << 30, bytes_accessed=1 << 20, transcendentals=0),
        compiler_params=pltpu.CompilerParams(collective_id=1, has_side_effects=True, vmem_limit_bytes=4 << 20),
        name="exchange",
    )(small)


def tail_kernel(G, s_ref, ids_ref, q_ref, o_ref, d_ref, send, recv):
    copies = send_all(G, s_ref, o_ref, send, recv)
    N, Q = q_ref.shape
    DL = Q // 3
    vb = 512

    def block(i, carry):
        rows = pl.ds(pl.multiple_of(i * vb, vb), vb)
        hot = lax.broadcasted_iota(jnp.int32, (vb, N), 0) + i * vb == ids_ref[...]
        d3 = jnp.dot(jnp.where(hot, 1.0, 0.0).astype(bf16), q_ref[...], preferred_element_type=f32)
        d_ref[rows, :] = d3[:, :DL] + d3[:, DL:2 * DL] + d3[:, 2 * DL:]
        return carry

    lax.fori_loop(0, d_ref.shape[0] // vb, block, 0)
    for cp in copies:
        cp.wait()


def tail(G, V, small, ids, q):
    vm = pl.BlockSpec(memory_space=pltpu.VMEM)
    return pl.pallas_call(
        functools.partial(tail_kernel, G),
        out_shape=(jax.ShapeDtypeStruct((G,) + small.shape, f32), jax.ShapeDtypeStruct((V, q.shape[1] // 3), f32)),
        in_specs=[vm, vm, vm],
        out_specs=(vm, vm),
        scratch_shapes=[pltpu.SemaphoreType.DMA((G - 1,)), pltpu.SemaphoreType.DMA((G - 1,))],
        cost_estimate=pl.CostEstimate(flops=2 * V * q.shape[0] * q.shape[1], bytes_accessed=6 << 20, transcendentals=0),
        compiler_params=pltpu.CompilerParams(collective_id=0, has_side_effects=True, vmem_limit_bytes=40 << 20),
        name="tail",
    )(small, ids, q)


def forward_kernel(last, DP, *refs):
    if last:
        (eb_ref, rs_ref, g_ref, w_ref, dh_ref, dl_ref, sr_ref, up_ref, ids_ref, _,
         dw_ref, xo_ref, u_ref, acc_ref, ub_ref) = refs
    else:
        (eb_ref, rs_ref, g_ref, w_ref, dh_ref, dl_ref, sr_ref, dw_ref, xo_ref, acc_ref) = refs
    j = pl.program_id(0)
    x = jnp.concatenate([eb_ref[i, 0] for i in range(DP)], axis=1)
    n = (x.astype(f32) * rs_ref[...] * g_ref[...]).astype(bf16)
    dw_ref[...] = (jnp.dot(n, dh_ref[...], preferred_element_type=f32)
                   + jnp.dot(n, dl_ref[...], preferred_element_type=f32))
    xo_ref[...] = jnp.dot(x, sr_ref[...], preferred_element_type=f32).T.astype(bf16)
    up = lax.dot_general(w_ref[...], n, (((0,), (0,)), ((), ())), preferred_element_type=f32)

    @pl.when(j == 0)
    def _():
        acc_ref[...] = up + up_ref[...] if last else up

    @pl.when(j > 0)
    def _():
        acc_ref[...] += up

    if last:
        @pl.when(j == pl.num_programs(0) - 1)
        def _():
            ub_ref[...] = acc_ref[...].astype(bf16)
            tb = 512

            def step(i, carry):
                rows = pl.ds(pl.multiple_of(i * tb, tb), tb)
                V = ub_ref.shape[1]
                hot = lax.broadcasted_iota(jnp.int32, (tb, V), 1) == ids_ref[rows, :]
                s = jnp.where(hot, 1.0, 0.0).astype(bf16)
                u_ref[rows, :] = lax.dot_general(s, ub_ref[...], (((1,), (1,)), ((), ())),
                                                 preferred_element_type=f32).astype(bf16)
                return carry

            lax.fori_loop(0, u_ref.shape[0] // tb, step, 0)


def forward(q, eb, rs, gcol, W, dh, dl, sr, up=None, ids=None, dw=None):
    last = q == 1
    DP, C, _, Vp = eb.shape
    V = DP * Vp
    D, FL = W.shape
    Dq = D // (2 * C)
    kt = 512
    nk = Dq // kt
    TS = sr.shape[1]
    base = q * C * nk
    one = pl.Buffered(1)

    def full(shape):
        return pl.BlockSpec(shape, lambda j: (0,) * len(shape), pipeline_mode=one)

    in_specs = [
        pl.BlockSpec((DP, 1, kt, Vp), lambda j: (0, j // nk, j % nk, 0)),
        full((1, V)),
        pl.BlockSpec((kt, 1), lambda j: (base + j, 0)),
        pl.BlockSpec((kt, FL), lambda j: (base + j, 0)),
        full((V, FL)), full((V, FL)), full((V, TS)),
    ]
    args = [eb, rs, gcol, W, dh, dl, sr]
    out_shape = [jax.ShapeDtypeStruct((D, FL), f32), jax.ShapeDtypeStruct((TS, D // 2), bf16)]
    out_specs = [pl.BlockSpec((kt, FL), lambda j: (base + j, 0)), pl.BlockSpec((TS, kt), lambda j: (0, j))]
    scratch = []
    alias = {}
    if last:
        N = ids.shape[0]
        in_specs += [full((FL, V)), full((N, 1)), pl.BlockSpec(memory_space=pl.ANY)]
        args += [up, ids, dw]
        alias = {9: 0}
        out_shape.append(jax.ShapeDtypeStruct((N, FL), bf16))
        out_specs.append(full((N, FL)))
        scratch = [pltpu.VMEM((FL, V), f32), pltpu.VMEM((FL, V), bf16)]
    else:
        out_shape.append(jax.ShapeDtypeStruct((FL, V), f32))
        out_specs.append(full((FL, V)))
    flops = 2 * V * FL * (D // 2) * 3 + (2 * V * V * FL if last else 0)
    return pl.pallas_call(
        functools.partial(forward_kernel, last, DP),
        grid=(C * nk,),
        in_specs=in_specs,
        out_specs=out_specs,
        out_shape=out_shape,
        scratch_shapes=scratch,
        input_output_aliases=alias,
        cost_estimate=pl.CostEstimate(flops=flops, bytes_accessed=30 << 20, transcendentals=0),
        compiler_params=pltpu.CompilerParams(dimension_semantics=("arbitrary",), vmem_limit_bytes=(52 if last else 40) << 20),
        name="forward",
    )(*args)


barrier = lax.optimization_barrier


def rows(a):
    return with_layout_constraint(a, Layout(major_to_minor=(0, 1)))


def split3(a):
    hi = lax.reduce_precision(a, 8, 7)
    mi = lax.reduce_precision(a - hi, 8, 7)
    lo = a - hi - mi
    return hi.astype(bf16), mi.astype(bf16), lo.astype(bf16)


def solution(mesh):
    G = mesh.shape['tp']
    DP = mesh.shape['dp']
    C = 2
    Z = G // C
    groups = [[d * G + z * C + c for d in range(DP) for c in range(C)] for z in range(Z)]

    def shift(k):
        return [(z * C + c, ((z + k) % Z) * C + c) for z in range(Z) for c in range(C)]

    swap = [(i, i ^ 1) for i in range(G)]

    def program(ids, E, g, W, du, dres):
        K, T = ids.shape
        N = K * T
        V, DL = E.shape
        D = g.shape[0]
        FL = W.shape[1]
        TL = T // G
        Vp = V // DP
        Dq = D // (2 * C)
        r = lax.axis_index('tp')
        grp = lax.axis_index('dp')
        z = r // C
        c = r % C
        gf = g.astype(f32)
        idf = ids.reshape(N)

        duf = du.reshape(N, FL)
        iota = jnp.arange(V, dtype=jnp.int32)

        Ep = lax.dynamic_slice_in_dim(E, grp * Vp, Vp, axis=0)
        AT = lax.all_gather(rows(Ep.T), 'tp', axis=0, tiled=True)

        du_o = lax.ppermute(duf, 'tp', swap)
        Ws = lax.dynamic_index_in_dim(W.reshape(Z, C, DL, FL), 1 - c, 1, False)
        W_o = lax.ppermute(Ws, 'tp', swap)
        gcol = gf.reshape(D, 1)
        du_o, W_o, gcol = barrier((du_o, W_o, gcol))
        F = Z // 2

        streams = [(0, 1, F), (1, -1, F), (1, 1, F - 1), (0, -1, F - 1)]
        acc = {0: [], 1: []}

        def hop(bufs):
            out = {}
            for st, b in bufs.items():
                out[st] = lax.ppermute(b, 'tp', shift(st[1]))
            return out

        def blocks(k):
            return [(s * (L - k), h) for h, s, L in streams if k < L]

        def add(moved, k, parts, hook):
            nxt = {}
            for (h, s, L), b in moved.items():
                if k == L:
                    acc[h].append(b)
                else:
                    b, _ = barrier((b, hook))
                    nxt[(h, s, L)] = b.astype(f32) + parts[(s * (L - k), h)]
            return nxt

        def chip(bl, Wo, dtype):
            return chip_parts(bl, z, c, Z, C, duf, du_o, W, Wo, dtype)

        p = chip(blocks(0), W_o, bf16)
        bufs = {(h, s, L): p[(s * L, h)] for h, s, L in streams}
        moved = hop(bufs)
        Wo1, _ = barrier((W_o, tuple(bufs.values())))
        p2 = chip(blocks(1), Wo1, f32)

        el = E.astype(f32)
        ssl = jnp.sum(el * el, axis=1)
        ssl, _ = barrier((ssl, tuple(p2.values())))
        ssg = exchange(G, ssl.reshape(V // 128, 128))
        rs2 = lax.rsqrt(jnp.sum(ssg, axis=0) / D + EPS).reshape(1, V)

        b1 = lax.dynamic_slice_in_dim(AT, c * Dq, Dq, axis=0)
        b2 = lax.dynamic_slice_in_dim(AT, D // 2 + c * Dq, Dq, axis=0)
        b1, b2 = barrier((rows(b1), rows(b2)))
        e1 = lax.all_gather(b1, ('dp', 'tp'), axis_index_groups=groups, axis=0, tiled=False).reshape(DP, C, Dq, Vp)
        e2 = lax.all_gather(b2, ('dp', 'tp'), axis_index_groups=groups, axis=0, tiled=False).reshape(DP, C, Dq, Vp)

        bufs = add(moved, 1, p2, b2)
        Wo2, _ = barrier((W_o, tuple(bufs.values())))
        moved = hop(bufs)
        p3 = chip([t for k in range(2, F) for t in blocks(k)] + [(0, 0), (0, 1)], Wo2, f32)
        idx, _ = barrier((idf, tuple(p3.values())))
        dh, dl, xl = rowsums(idx.reshape(1, N), duf, E)
        rst = jnp.sum(jnp.where(idx[:, None] == iota[None, :], rs2, 0.0), axis=1)
        idr = lax.dynamic_slice_in_dim(ids, r * TL, TL, axis=1).reshape(K * TL)
        sr = (iota[:, None] == idr[None, :]).astype(bf16)
        idc = idx.reshape(N, 1)
        rs2, sr, idc, xl, rst = barrier((rs2, sr, idc, xl, rst))

        bufs = add(moved, 2, p3, xl)
        rs2, _ = barrier((rs2, tuple(bufs.values())))
        moved = hop(bufs)
        drs, _ = barrier((dres, tuple(bufs.values())))
        dc = lax.all_to_all(drs.reshape(K, TL, G, DL), 'tp', 2, 0, tiled=False)
        dresc = dc.reshape(G, K, TL, DL).transpose(1, 0, 2, 3).reshape(N, DL)
        dw1, x1, up = forward(0, e1, rs2, gcol, W, dh, dl, sr)
        for k in range(3, F):
            bufs = add(moved, k, p3, x1)
            rs2, _ = barrier((rs2, tuple(bufs.values())))
            moved = hop(bufs)
        dW, x2, u = forward(1, e2, rs2, gcol, W, dh, dl, sr, up, idc, dw1)
        moved = {st: barrier((b, x2))[0] for st, b in moved.items()}
        add(moved, F, p3, x2)
        dn = jnp.concatenate([p3[(0, h)] + sum(b.astype(f32) for b in acc[h]) for h in (0, 1)], axis=0)
        xo = jnp.concatenate([x1, x2], axis=1).reshape(K, TL, D)
        u = u.reshape(K, T, FL)

        gl = lax.dynamic_slice_in_dim(gf, r * DL, DL)
        nh = xl.astype(f32) * rst[:, None]
        gdn = gl * dn
        sp = jnp.sum(nh * gdn, axis=1)
        dgl = jnp.sum(dn * nh, axis=0)
        small = jnp.concatenate([sp, dgl]).reshape((N + DL) // 128, 128)
        q = jnp.concatenate(split3(dresc.astype(f32) + rst[:, None] * gdn), axis=1)
        small, dA = tail(G, V, small, idx.reshape(1, N), q)
        small = small.reshape(G, N + DL)
        s = jnp.sum(small[:, :N], axis=0) / D
        dg = small[:, N:].reshape(D)
        sv = jnp.sum(jnp.where(iota[:, None] == idf[None, :], s[None, :], 0.0), axis=1)
        rv = rs2.reshape(V, 1)
        dE = dA - rv * (E.astype(f32) * rv) * sv[:, None]
        return u, xo, dE, dW, dg

    return jax.shard_map(
        program,
        mesh=mesh,
        in_specs=(P('dp', None), P(None, 'tp'), P(), P(None, 'tp'), P('dp', None, 'tp'), P('dp', 'tp', None)),
        out_specs=(P('dp', None, 'tp'), P('dp', 'tp', None), P('dp', 'tp'), P('dp', 'tp'), P('dp')),
        check_vma=False,
    )
```

```python
import functools

import jax
import jax.numpy as jnp
from jax import lax
from jax.experimental import pallas as pl
from jax.experimental.layout import Layout, with_layout_constraint
from jax.experimental.pallas import tpu as pltpu
from jax.sharding import PartitionSpec as P


EPS = 1e-6
MESH = pl.DeviceIdType.MESH
f32 = jnp.float32
bf16 = jnp.bfloat16


def parts_kernel(nb, idx_ref, a_ref, b_ref, wa_ref, wb_ref, *outs):
    nt = (((1,), (1,)), ((), ()))
    o = (lax.dot_general(a_ref[...], wa_ref[...], nt, preferred_element_type=f32)
         + lax.dot_general(b_ref[...], wb_ref[...], nt, preferred_element_type=f32)).astype(outs[0].dtype)
    for i in range(nb):
        @pl.when(pl.program_id(0) == i)
        def _(i=i):
            outs[i][...] = o


def chip_parts(blocks, z, c, Z, C, a, b, W, Wo, dtype):
    blocks = sorted(blocks, key=lambda t: t[1])
    nb = len(blocks)
    N, FL = a.shape
    DL = Wo.shape[1]
    M = N // 2
    zd = [lax.rem(z + d + Z, Z) for d, _ in blocks]
    idx = jnp.stack([q * C + c for q in zd] + zd)
    first = sum(1 for _, h in blocks if h == 0)
    row = lambda i, s: (jnp.where(i >= first, 1, 0), 0)
    outs = pl.pallas_call(
        functools.partial(parts_kernel, nb),
        grid_spec=pltpu.PrefetchScalarGridSpec(
            num_scalar_prefetch=1,
            grid=(nb,),
            in_specs=[
                pl.BlockSpec((M, FL), row), pl.BlockSpec((M, FL), row),
                pl.BlockSpec((DL, FL), lambda i, s: (s[i], 0)), pl.BlockSpec((DL, FL), lambda i, s: (s[nb + i], 0)),
            ],
            out_specs=[pl.BlockSpec((M, DL), lambda i, s: (0, 0)) for _ in blocks],
        ),
        out_shape=[jax.ShapeDtypeStruct((M, DL), dtype) for _ in blocks],
        cost_estimate=pl.CostEstimate(flops=4 * M * DL * FL * nb, bytes_accessed=8 << 20, transcendentals=0),
        compiler_params=pltpu.CompilerParams(dimension_semantics=("arbitrary",), vmem_limit_bytes=62 << 20),
        name="chip_parts",
    )(idx, a, b, W, Wo.reshape(-1, FL))
    return dict(zip(blocks, outs))


def rowsum_kernel(ids_ref, du_ref, e_ref, hi_ref, lo_ref, x_ref, acc_ref):
    i = pl.program_id(0)
    vb = e_ref.shape[0]
    hot = lax.broadcasted_iota(jnp.int32, (vb, du_ref.shape[0]), 0) + i * vb == ids_ref[...]
    hot = jnp.where(hot, 1.0, 0.0).astype(bf16)
    d = jnp.dot(hot, du_ref[...], preferred_element_type=f32)
    hi = d.astype(bf16)
    hi_ref[...] = hi
    lo_ref[...] = (d - hi.astype(f32)).astype(bf16)

    @pl.when(i == 0)
    def _():
        acc_ref[...] = jnp.zeros(acc_ref.shape, f32)

    acc_ref[...] += lax.dot_general(hot, e_ref[...], (((0,), (0,)), ((), ())), preferred_element_type=f32)

    @pl.when(i == pl.num_programs(0) - 1)
    def _():
        x_ref[...] = acc_ref[...].astype(bf16)


def rowsums(ids, du, E):
    N, FL = du.shape
    V, DL = E.shape
    vb = 512
    one = pl.Buffered(1)
    return pl.pallas_call(
        rowsum_kernel,
        grid=(V // vb,),
        in_specs=[
            pl.BlockSpec((1, N), lambda i: (0, 0)),
            pl.BlockSpec((N, FL), lambda i: (0, 0), pipeline_mode=one),
            pl.BlockSpec((vb, DL), lambda i: (i, 0)),
        ],
        out_specs=[pl.BlockSpec((vb, FL), lambda i: (i, 0)), pl.BlockSpec((vb, FL), lambda i: (i, 0)),
                   pl.BlockSpec((N, DL), lambda i: (0, 0))],
        out_shape=[jax.ShapeDtypeStruct((V, FL), bf16), jax.ShapeDtypeStruct((V, FL), bf16),
                   jax.ShapeDtypeStruct((N, DL), bf16)],
        scratch_shapes=[pltpu.VMEM((N, DL), f32)],
        cost_estimate=pl.CostEstimate(flops=2 * V * N * (FL + DL), bytes_accessed=12 << 20, transcendentals=0),
        compiler_params=pltpu.CompilerParams(dimension_semantics=("arbitrary",), vmem_limit_bytes=62 << 20),
        name="rowsums",
    )(ids, du, E)


def send_all(G, s_ref, o_ref, send, recv):
    me = lax.axis_index('tp')
    bar = pltpu.get_barrier_semaphore()
    for k in range(1, G):
        pl.semaphore_signal(bar, inc=1, device_id={'tp': lax.rem(me + k, G)}, device_id_type=MESH)
    pl.semaphore_wait(bar, G - 1)
    copies = []
    for k in range(1, G):
        cp = pltpu.make_async_remote_copy(
            src_ref=s_ref, dst_ref=o_ref.at[me], send_sem=send.at[k - 1], recv_sem=recv.at[k - 1],
            device_id={'tp': lax.rem(me + k, G)}, device_id_type=MESH)
        cp.start()
        copies.append(cp)
    o_ref[me] = s_ref[...]
    return copies


def exchange_kernel(G, s_ref, o_ref, send, recv):
    for cp in send_all(G, s_ref, o_ref, send, recv):
        cp.wait()


def exchange(G, small):
    vm = pl.BlockSpec(memory_space=pltpu.VMEM)
    return pl.pallas_call(
        functools.partial(exchange_kernel, G),
        out_shape=jax.ShapeDtypeStruct((G,) + small.shape, f32),
        in_specs=[vm],
        out_specs=vm,
        scratch_shapes=[pltpu.SemaphoreType.DMA((G - 1,)), pltpu.SemaphoreType.DMA((G - 1,))],
        cost_estimate=pl.CostEstimate(flops=1 << 30, bytes_accessed=1 << 20, transcendentals=0),
        compiler_params=pltpu.CompilerParams(collective_id=1, has_side_effects=True, vmem_limit_bytes=4 << 20),
        name="exchange",
    )(small)


def tail_kernel(G, s_ref, ids_ref, q_ref, o_ref, d_ref, send, recv):
    copies = send_all(G, s_ref, o_ref, send, recv)
    N, Q = q_ref.shape
    DL = Q // 3
    vb = 512

    def block(i, carry):
        rows = pl.ds(pl.multiple_of(i * vb, vb), vb)
        hot = lax.broadcasted_iota(jnp.int32, (vb, N), 0) + i * vb == ids_ref[...]
        d3 = jnp.dot(jnp.where(hot, 1.0, 0.0).astype(bf16), q_ref[...], preferred_element_type=f32)
        d_ref[rows, :] = d3[:, :DL] + d3[:, DL:2 * DL] + d3[:, 2 * DL:]
        return carry

    lax.fori_loop(0, d_ref.shape[0] // vb, block, 0)
    for cp in copies:
        cp.wait()


def tail(G, V, small, ids, q):
    vm = pl.BlockSpec(memory_space=pltpu.VMEM)
    return pl.pallas_call(
        functools.partial(tail_kernel, G),
        out_shape=(jax.ShapeDtypeStruct((G,) + small.shape, f32), jax.ShapeDtypeStruct((V, q.shape[1] // 3), f32)),
        in_specs=[vm, vm, vm],
        out_specs=(vm, vm),
        scratch_shapes=[pltpu.SemaphoreType.DMA((G - 1,)), pltpu.SemaphoreType.DMA((G - 1,))],
        cost_estimate=pl.CostEstimate(flops=2 * V * q.shape[0] * q.shape[1], bytes_accessed=6 << 20, transcendentals=0),
        compiler_params=pltpu.CompilerParams(collective_id=0, has_side_effects=True, vmem_limit_bytes=40 << 20),
        name="tail",
    )(small, ids, q)


def forward_kernel(last, DP, *refs):
    if last:
        (eb_ref, rs_ref, g_ref, w_ref, dh_ref, dl_ref, sr_ref, up_ref, ids_ref, _,
         dw_ref, xo_ref, u_ref, acc_ref, ub_ref) = refs
    else:
        (eb_ref, rs_ref, g_ref, w_ref, dh_ref, dl_ref, sr_ref, dw_ref, xo_ref, acc_ref) = refs
    j = pl.program_id(0)
    x = jnp.concatenate([eb_ref[i, 0] for i in range(DP)], axis=1)
    n = (x.astype(f32) * rs_ref[...] * g_ref[...]).astype(bf16)
    dw_ref[...] = (jnp.dot(n, dh_ref[...], preferred_element_type=f32)
                   + jnp.dot(n, dl_ref[...], preferred_element_type=f32))
    xo_ref[...] = jnp.dot(x, sr_ref[...], preferred_element_type=f32).T.astype(bf16)

    @pl.when(j == 0)
    def _():
        acc_ref[...] = up_ref[...] if last else jnp.zeros(acc_ref.shape, f32)

    acc_ref[...] += lax.dot_general(w_ref[...], n, (((0,), (0,)), ((), ())), preferred_element_type=f32)

    if last:
        @pl.when(j == pl.num_programs(0) - 1)
        def _():
            ub_ref[...] = acc_ref[...].astype(bf16)
            tb = 512

            def step(i, carry):
                rows = pl.ds(pl.multiple_of(i * tb, tb), tb)
                V = ub_ref.shape[1]
                hot = lax.broadcasted_iota(jnp.int32, (tb, V), 1) == ids_ref[rows, :]
                s = jnp.where(hot, 1.0, 0.0).astype(bf16)
                u_ref[rows, :] = lax.dot_general(s, ub_ref[...], (((1,), (1,)), ((), ())),
                                                 preferred_element_type=f32).astype(bf16)
                return carry

            lax.fori_loop(0, u_ref.shape[0] // tb, step, 0)


def forward(row0, eb, rs, gcol, W, dh, dl, sr, up=None, ids=None, dw=None):
    last = up is not None
    DP, C, R, Vp = eb.shape
    V = DP * Vp
    D, FL = W.shape
    kt = 512
    nk = R // kt
    TS = sr.shape[1]
    base = row0 // kt
    one = pl.Buffered(1)

    def full(shape):
        return pl.BlockSpec(shape, lambda j: (0,) * len(shape), pipeline_mode=one)

    in_specs = [
        pl.BlockSpec((DP, 1, kt, Vp), lambda j: (0, j // nk, j % nk, 0)),
        full((1, V)),
        pl.BlockSpec((kt, 1), lambda j: (base + j, 0)),
        pl.BlockSpec((kt, FL), lambda j: (base + j, 0)),
        full((V, FL)), full((V, FL)), full((V, TS)),
    ]
    args = [eb, rs, gcol, W, dh, dl, sr]
    out_shape = [jax.ShapeDtypeStruct((D, FL), f32), jax.ShapeDtypeStruct((TS, C * R), bf16)]
    out_specs = [pl.BlockSpec((kt, FL), lambda j: (base + j, 0)), pl.BlockSpec((TS, kt), lambda j: (0, j))]
    scratch = []
    alias = {}
    if last:
        N = ids.shape[0]
        in_specs += [full((FL, V)), full((N, 1)), pl.BlockSpec(memory_space=pl.ANY)]
        args += [up, ids, dw]
        alias = {9: 0}
        out_shape.append(jax.ShapeDtypeStruct((N, FL), bf16))
        out_specs.append(full((N, FL)))
        scratch = [pltpu.VMEM((FL, V), f32), pltpu.VMEM((FL, V), bf16)]
    else:
        out_shape.append(jax.ShapeDtypeStruct((FL, V), f32))
        out_specs.append(full((FL, V)))
    flops = 2 * V * FL * C * R * 3 + (2 * V * V * FL if last else 0)
    return pl.pallas_call(
        functools.partial(forward_kernel, last, DP),
        grid=(C * nk,),
        in_specs=in_specs,
        out_specs=out_specs,
        out_shape=out_shape,
        scratch_shapes=scratch,
        input_output_aliases=alias,
        cost_estimate=pl.CostEstimate(flops=flops, bytes_accessed=30 << 20, transcendentals=0),
        compiler_params=pltpu.CompilerParams(dimension_semantics=("arbitrary",), vmem_limit_bytes=62 << 20),
        name="forward",
    )(*args)


barrier = lax.optimization_barrier


def rows(a):
    return with_layout_constraint(a, Layout(major_to_minor=(0, 1)))


def split3(a):
    hi = lax.reduce_precision(a, 8, 7)
    mi = lax.reduce_precision(a - hi, 8, 7)
    lo = a - hi - mi
    return hi.astype(bf16), mi.astype(bf16), lo.astype(bf16)


def solution(mesh):
    G = mesh.shape['tp']
    DP = mesh.shape['dp']
    C = 2
    Z = G // C
    groups = [[d * G + z * C + c for d in range(DP) for c in range(C)] for z in range(Z)]

    def shift(k):
        return [(z * C + c, ((z + k) % Z) * C + c) for z in range(Z) for c in range(C)]

    swap = [(i, i ^ 1) for i in range(G)]

    def program(ids, E, g, W, du, dres):
        K, T = ids.shape
        N = K * T
        V, DL = E.shape
        D = g.shape[0]
        FL = W.shape[1]
        TL = T // G
        Vp = V // DP
        D1 = 3 * D // 4
        R1, R2 = D1 // C, (D - D1) // C
        r = lax.axis_index('tp')
        grp = lax.axis_index('dp')
        z = r // C
        c = r % C
        gf = g.astype(f32)
        idf = ids.reshape(N)

        duf = du.reshape(N, FL)
        iota = jnp.arange(V, dtype=jnp.int32)

        Ep = lax.dynamic_slice_in_dim(E, grp * Vp, Vp, axis=0)
        AT = lax.all_gather(rows(Ep.T), 'tp', axis=0, tiled=True)

        du_o = lax.ppermute(duf, 'tp', swap)
        Ws = lax.dynamic_index_in_dim(W.reshape(Z, C, DL, FL), 1 - c, 1, False)
        W_o = lax.ppermute(Ws, 'tp', swap)
        el = E.astype(f32)
        ssl = jnp.sum(el * el, axis=1)
        ssl, _ = barrier((ssl, Ws))
        ssg = exchange(G, ssl.reshape(V // 128, 128))
        rs2 = lax.rsqrt(jnp.sum(ssg, axis=0) / D + EPS).reshape(1, V)
        gcol = gf.reshape(D, 1)
        du_o, W_o, gcol, rs2 = barrier((du_o, W_o, gcol, rs2))
        F = Z // 2

        streams = [(0, 1, F), (1, -1, F), (1, 1, F - 1), (0, -1, F - 1)]
        acc = {0: [], 1: []}

        def hop(bufs):
            out = {}
            for st, b in bufs.items():
                out[st] = lax.ppermute(b, 'tp', shift(st[1]))
            return out

        def blocks(k):
            return [(s * (L - k), h) for h, s, L in streams if k < L]

        def add(moved, k, parts, hook):
            nxt = {}
            for (h, s, L), b in moved.items():
                if k == L:
                    acc[h].append(b)
                else:
                    b, _ = barrier((b, hook))
                    nxt[(h, s, L)] = b.astype(f32) + parts[(s * (L - k), h)]
            return nxt

        def chip(bl, Wo, dtype):
            return chip_parts(bl, z, c, Z, C, duf, du_o, W, Wo, dtype)

        p = chip(blocks(0), W_o, bf16)
        bufs = {(h, s, L): p[(s * L, h)] for h, s, L in streams}
        moved = hop(bufs)
        Wo1, _ = barrier((W_o, tuple(bufs.values())))
        p2 = chip(blocks(1), Wo1, f32)

        b1 = lax.dynamic_slice_in_dim(AT, c * R1, R1, axis=0)
        b2 = lax.dynamic_slice_in_dim(AT, D1 + c * R2, R2, axis=0)
        b1, b2 = barrier((rows(b1), rows(b2)))
        e1 = lax.all_gather(b1, ('dp', 'tp'), axis_index_groups=groups, axis=0, tiled=False).reshape(DP, C, R1, Vp)
        e2 = lax.all_gather(b2, ('dp', 'tp'), axis_index_groups=groups, axis=0, tiled=False).reshape(DP, C, R2, Vp)

        bufs = add(moved, 1, p2, b2)
        Wo2, _ = barrier((W_o, tuple(bufs.values())))
        moved = hop(bufs)
        p3 = chip([t for k in range(2, F) for t in blocks(k)] + [(0, 0), (0, 1)], Wo2, f32)
        idx, _ = barrier((idf, tuple(p3.values())))
        dh, dl, xl = rowsums(idx.reshape(1, N), duf, E)
        rst = jnp.sum(jnp.where(idx[:, None] == iota[None, :], rs2, 0.0), axis=1)
        idr = lax.dynamic_slice_in_dim(ids, r * TL, TL, axis=1).reshape(K * TL)
        sr = (iota[:, None] == idr[None, :]).astype(bf16)
        idc = idf.reshape(N, 1)
        rs2, sr, idc, xl, rst = barrier((rs2, sr, idc, xl, rst))

        bufs = add(moved, 2, p3, xl)
        rs2, _ = barrier((rs2, tuple(bufs.values())))
        moved = hop(bufs)
        drs, _ = barrier((dres, tuple(bufs.values())))
        dc = lax.all_to_all(drs.reshape(K, TL, G, DL), 'tp', 2, 0, tiled=False)
        dw1, x1, up = forward(0, e1, rs2, gcol, W, dh, dl, sr)
        for k in range(3, F):
            bufs = add(moved, k, p3, x1)
            rs2, _ = barrier((rs2, tuple(bufs.values())))
            moved = hop(bufs)
        dW, x2, u = forward(D1, e2, rs2, gcol, W, dh, dl, sr, up, idc, dw1)
        moved = {st: barrier((b, x2))[0] for st, b in moved.items()}
        dc, _ = barrier((dc, x2))
        dresc = dc.reshape(G, K, TL, DL).transpose(1, 0, 2, 3).reshape(N, DL)
        add(moved, F, p3, x2)
        dn = jnp.concatenate([p3[(0, h)] + sum(b.astype(f32) for b in acc[h]) for h in (0, 1)], axis=0)
        xo = jnp.concatenate([x1, x2], axis=1).reshape(K, TL, D)
        u = u.reshape(K, T, FL)

        gl = lax.dynamic_slice_in_dim(gf, r * DL, DL)
        nh = xl.astype(f32) * rst[:, None]
        gdn = gl * dn
        sp = jnp.sum(nh * gdn, axis=1)
        dgl = jnp.sum(dn * nh, axis=0)
        small = jnp.concatenate([sp, dgl]).reshape((N + DL) // 128, 128)
        q = jnp.concatenate(split3(dresc.astype(f32) + rst[:, None] * gdn), axis=1)
        small, dA = tail(G, V, small, idx.reshape(1, N), q)
        small = small.reshape(G, N + DL)
        s = jnp.sum(small[:, :N], axis=0) / D
        dg = small[:, N:].reshape(D)
        sv = jnp.sum(jnp.where(iota[:, None] == idf[None, :], s[None, :], 0.0), axis=1)
        rv = rs2.reshape(V, 1)
        dE = dA - rv * (E.astype(f32) * rv) * sv[:, None]
        return u, xo, dE, dW, dg

    return jax.shard_map(
        program,
        mesh=mesh,
        in_specs=(P('dp', None), P(None, 'tp'), P(), P(None, 'tp'), P('dp', None, 'tp'), P('dp', 'tp', None)),
        out_specs=(P('dp', None, 'tp'), P('dp', 'tp', None), P('dp', 'tp'), P('dp', 'tp'), P('dp')),
        check_vma=False,
    )
```

```python
import functools

import jax
import jax.numpy as jnp
from jax import lax
from jax.experimental import pallas as pl
from jax.experimental.layout import Layout, with_layout_constraint
from jax.experimental.pallas import tpu as pltpu
from jax.sharding import PartitionSpec as P


EPS = 1e-6
MESH = pl.DeviceIdType.MESH
f32 = jnp.float32
bf16 = jnp.bfloat16


def parts_kernel(nb, idx_ref, a_ref, b_ref, wa_ref, wb_ref, *outs):
    nt = (((1,), (1,)), ((), ()))
    o = (lax.dot_general(a_ref[...], wa_ref[...], nt, preferred_element_type=f32)
         + lax.dot_general(b_ref[...], wb_ref[...], nt, preferred_element_type=f32)).astype(outs[0].dtype)
    for i in range(nb):
        @pl.when(pl.program_id(0) == i)
        def _(i=i):
            outs[i][...] = o


def chip_parts(blocks, z, c, Z, C, a, b, W, Wo, dtype):
    blocks = sorted(blocks, key=lambda t: t[1])
    nb = len(blocks)
    N, FL = a.shape
    DL = Wo.shape[1]
    M = N // 2
    zd = [lax.rem(z + d + Z, Z) for d, _ in blocks]
    idx = jnp.stack([q * C + c for q in zd] + zd)
    first = sum(1 for _, h in blocks if h == 0)
    row = lambda i, s: (jnp.where(i >= first, 1, 0), 0)
    outs = pl.pallas_call(
        functools.partial(parts_kernel, nb),
        grid_spec=pltpu.PrefetchScalarGridSpec(
            num_scalar_prefetch=1,
            grid=(nb,),
            in_specs=[
                pl.BlockSpec((M, FL), row), pl.BlockSpec((M, FL), row),
                pl.BlockSpec((DL, FL), lambda i, s: (s[i], 0)), pl.BlockSpec((DL, FL), lambda i, s: (s[nb + i], 0)),
            ],
            out_specs=[pl.BlockSpec((M, DL), lambda i, s: (0, 0)) for _ in blocks],
        ),
        out_shape=[jax.ShapeDtypeStruct((M, DL), dtype) for _ in blocks],
        cost_estimate=pl.CostEstimate(flops=4 * M * DL * FL * nb, bytes_accessed=8 << 20, transcendentals=0),
        compiler_params=pltpu.CompilerParams(dimension_semantics=("arbitrary",), vmem_limit_bytes=62 << 20),
        name="chip_parts",
    )(idx, a, b, W, Wo.reshape(-1, FL))
    return dict(zip(blocks, outs))


def rowsum_kernel(ids_ref, du_ref, e_ref, hi_ref, lo_ref, x_ref, acc_ref):
    i = pl.program_id(0)
    vb = e_ref.shape[0]
    hot = lax.broadcasted_iota(jnp.int32, (vb, du_ref.shape[0]), 0) + i * vb == ids_ref[...]
    hot = jnp.where(hot, 1.0, 0.0).astype(bf16)
    d = jnp.dot(hot, du_ref[...], preferred_element_type=f32)
    hi = d.astype(bf16)
    hi_ref[...] = hi
    lo_ref[...] = (d - hi.astype(f32)).astype(bf16)

    @pl.when(i == 0)
    def _():
        acc_ref[...] = jnp.zeros(acc_ref.shape, f32)

    acc_ref[...] += lax.dot_general(hot, e_ref[...], (((0,), (0,)), ((), ())), preferred_element_type=f32)

    @pl.when(i == pl.num_programs(0) - 1)
    def _():
        x_ref[...] = acc_ref[...].astype(bf16)


def rowsums(ids, du, E):
    N, FL = du.shape
    V, DL = E.shape
    vb = 512
    one = pl.Buffered(1)
    return pl.pallas_call(
        rowsum_kernel,
        grid=(V // vb,),
        in_specs=[
            pl.BlockSpec((1, N), lambda i: (0, 0)),
            pl.BlockSpec((N, FL), lambda i: (0, 0), pipeline_mode=one),
            pl.BlockSpec((vb, DL), lambda i: (i, 0)),
        ],
        out_specs=[pl.BlockSpec((vb, FL), lambda i: (i, 0)), pl.BlockSpec((vb, FL), lambda i: (i, 0)),
                   pl.BlockSpec((N, DL), lambda i: (0, 0))],
        out_shape=[jax.ShapeDtypeStruct((V, FL), bf16), jax.ShapeDtypeStruct((V, FL), bf16),
                   jax.ShapeDtypeStruct((N, DL), bf16)],
        scratch_shapes=[pltpu.VMEM((N, DL), f32)],
        cost_estimate=pl.CostEstimate(flops=2 * V * N * (FL + DL), bytes_accessed=12 << 20, transcendentals=0),
        compiler_params=pltpu.CompilerParams(dimension_semantics=("arbitrary",), vmem_limit_bytes=62 << 20),
        name="rowsums",
    )(ids, du, E)


def send_all(G, s_ref, o_ref, send, recv):
    me = lax.axis_index('tp')
    bar = pltpu.get_barrier_semaphore()
    for k in range(1, G):
        pl.semaphore_signal(bar, inc=1, device_id={'tp': lax.rem(me + k, G)}, device_id_type=MESH)
    pl.semaphore_wait(bar, G - 1)
    copies = []
    for k in range(1, G):
        cp = pltpu.make_async_remote_copy(
            src_ref=s_ref, dst_ref=o_ref.at[me], send_sem=send.at[k - 1], recv_sem=recv.at[k - 1],
            device_id={'tp': lax.rem(me + k, G)}, device_id_type=MESH)
        cp.start()
        copies.append(cp)
    o_ref[me] = s_ref[...]
    return copies


def exchange_kernel(G, s_ref, o_ref, send, recv):
    for cp in send_all(G, s_ref, o_ref, send, recv):
        cp.wait()


def exchange(G, small):
    vm = pl.BlockSpec(memory_space=pltpu.VMEM)
    return pl.pallas_call(
        functools.partial(exchange_kernel, G),
        out_shape=jax.ShapeDtypeStruct((G,) + small.shape, f32),
        in_specs=[vm],
        out_specs=vm,
        scratch_shapes=[pltpu.SemaphoreType.DMA((G - 1,)), pltpu.SemaphoreType.DMA((G - 1,))],
        cost_estimate=pl.CostEstimate(flops=1 << 30, bytes_accessed=1 << 20, transcendentals=0),
        compiler_params=pltpu.CompilerParams(collective_id=1, has_side_effects=True, vmem_limit_bytes=4 << 20),
        name="exchange",
    )(small)


def tail_kernel(G, s_ref, ids_ref, q_ref, o_ref, d_ref, send, recv):
    copies = send_all(G, s_ref, o_ref, send, recv)
    N, Q = q_ref.shape
    DL = Q // 3
    vb = 512

    def block(i, carry):
        rows = pl.ds(pl.multiple_of(i * vb, vb), vb)
        hot = lax.broadcasted_iota(jnp.int32, (vb, N), 0) + i * vb == ids_ref[...]
        d3 = jnp.dot(jnp.where(hot, 1.0, 0.0).astype(bf16), q_ref[...], preferred_element_type=f32)
        d_ref[rows, :] = d3[:, :DL] + d3[:, DL:2 * DL] + d3[:, 2 * DL:]
        return carry

    lax.fori_loop(0, d_ref.shape[0] // vb, block, 0)
    for cp in copies:
        cp.wait()


def tail(G, V, small, ids, q):
    vm = pl.BlockSpec(memory_space=pltpu.VMEM)
    return pl.pallas_call(
        functools.partial(tail_kernel, G),
        out_shape=(jax.ShapeDtypeStruct((G,) + small.shape, f32), jax.ShapeDtypeStruct((V, q.shape[1] // 3), f32)),
        in_specs=[vm, vm, vm],
        out_specs=(vm, vm),
        scratch_shapes=[pltpu.SemaphoreType.DMA((G - 1,)), pltpu.SemaphoreType.DMA((G - 1,))],
        cost_estimate=pl.CostEstimate(flops=2 * V * q.shape[0] * q.shape[1], bytes_accessed=6 << 20, transcendentals=0),
        compiler_params=pltpu.CompilerParams(collective_id=0, has_side_effects=True, vmem_limit_bytes=40 << 20),
        name="tail",
    )(small, ids, q)


def forward_kernel(last, DP, *refs):
    if last:
        (eb_ref, rs_ref, g_ref, w_ref, dh_ref, dl_ref, sr_ref, up_ref, ids_ref, _, _,
         dw_ref, xo_ref, u_ref, acc_ref, n_ref) = refs
    else:
        (eb_ref, rs_ref, g_ref, w_ref, dh_ref, dl_ref, sr_ref, dw_ref, xo_ref, acc_ref, n_ref) = refs
    j = pl.program_id(0)
    kt, V = n_ref.shape

    @pl.when(j == 0)
    def _():
        acc_ref[...] = up_ref[...] if last else jnp.zeros(acc_ref.shape, f32)

    ck = 512
    for h in range(kt // ck):
        rows = slice(h * ck, (h + 1) * ck)
        x = jnp.concatenate([eb_ref[i, 0, rows, :] for i in range(DP)], axis=1)
        n_ref[rows, :] = (x.astype(f32) * rs_ref[...] * g_ref[rows, :]).astype(bf16)
        xo_ref[:, rows] = jnp.dot(x, sr_ref[...], preferred_element_type=f32).T.astype(bf16)
    dw_ref[...] = (jnp.dot(n_ref[...], dh_ref[...], preferred_element_type=f32)
                   + jnp.dot(n_ref[...], dl_ref[...], preferred_element_type=f32))
    acc_ref[...] += lax.dot_general(w_ref[...], n_ref[...], (((0,), (0,)), ((), ())), preferred_element_type=f32)

    if last:
        @pl.when(j == pl.num_programs(0) - 1)
        def _():
            FL = acc_ref.shape[0]
            n_ref[:FL, :] = acc_ref[...].astype(bf16)
            tb = 512

            def step(i, carry):
                rows = pl.ds(pl.multiple_of(i * tb, tb), tb)
                hot = lax.broadcasted_iota(jnp.int32, (tb, V), 1) == ids_ref[rows, :]
                s = jnp.where(hot, 1.0, 0.0).astype(bf16)
                u_ref[rows, :] = lax.dot_general(s, n_ref[:FL, :], (((1,), (1,)), ((), ())),
                                                 preferred_element_type=f32).astype(bf16)
                return carry

            lax.fori_loop(0, u_ref.shape[0] // tb, step, 0)


def forward(row0, eb, rs, gcol, W, dh, dl, sr, up=None, ids=None, dw=None, xo=None):
    last = up is not None
    DP, C, R, Vp = eb.shape
    V = DP * Vp
    D, FL = W.shape
    kt = 1024
    nk = R // kt
    TS = sr.shape[1]
    base = row0 // kt
    one = pl.Buffered(1)

    def full(shape):
        return pl.BlockSpec(shape, lambda j: (0,) * len(shape), pipeline_mode=one)

    in_specs = [
        pl.BlockSpec((DP, 1, kt, Vp), lambda j: (0, j // nk, j % nk, 0)),
        full((1, V)),
        pl.BlockSpec((kt, 1), lambda j: (base + j, 0)),
        pl.BlockSpec((kt, FL), lambda j: (base + j, 0)),
        full((V, FL)), full((V, FL)), full((V, TS)),
    ]
    args = [eb, rs, gcol, W, dh, dl, sr]
    out_shape = [jax.ShapeDtypeStruct((D, FL), f32), jax.ShapeDtypeStruct((TS, D), bf16)]
    out_specs = [pl.BlockSpec((kt, FL), lambda j: (base + j, 0)), pl.BlockSpec((TS, kt), lambda j: (0, base + j))]
    scratch = [pltpu.VMEM((kt, V), bf16)]
    alias = {}
    if last:
        N = ids.shape[0]
        in_specs += [full((FL, V)), full((N, 1)), pl.BlockSpec(memory_space=pl.ANY), pl.BlockSpec(memory_space=pl.ANY)]
        args += [up, ids, dw, xo]
        alias = {9: 0, 10: 1}
        out_shape.append(jax.ShapeDtypeStruct((N, FL), bf16))
        out_specs.append(full((N, FL)))
        scratch = [pltpu.VMEM((FL, V), f32)] + scratch
    else:
        out_shape.append(jax.ShapeDtypeStruct((FL, V), f32))
        out_specs.append(full((FL, V)))
    flops = 2 * V * FL * C * R * 3 + (2 * V * V * FL if last else 0)
    return pl.pallas_call(
        functools.partial(forward_kernel, last, DP),
        grid=(C * nk,),
        in_specs=in_specs,
        out_specs=out_specs,
        out_shape=out_shape,
        scratch_shapes=scratch,
        input_output_aliases=alias,
        cost_estimate=pl.CostEstimate(flops=flops, bytes_accessed=30 << 20, transcendentals=0),
        compiler_params=pltpu.CompilerParams(dimension_semantics=("arbitrary",), vmem_limit_bytes=62 << 20),
        name="forward",
    )(*args)


barrier = lax.optimization_barrier


def rows(a):
    return with_layout_constraint(a, Layout(major_to_minor=(0, 1)))


def split3(a):
    hi = lax.reduce_precision(a, 8, 7)
    mi = lax.reduce_precision(a - hi, 8, 7)
    lo = a - hi - mi
    return hi.astype(bf16), mi.astype(bf16), lo.astype(bf16)


def solution(mesh):
    G = mesh.shape['tp']
    DP = mesh.shape['dp']
    C = 2
    Z = G // C
    groups = [[d * G + z * C + c for d in range(DP) for c in range(C)] for z in range(Z)]

    def shift(k):
        return [(z * C + c, ((z + k) % Z) * C + c) for z in range(Z) for c in range(C)]

    swap = [(i, i ^ 1) for i in range(G)]

    def program(ids, E, g, W, du, dres):
        K, T = ids.shape
        N = K * T
        V, DL = E.shape
        D = g.shape[0]
        FL = W.shape[1]
        TL = T // G
        Vp = V // DP
        D1 = D // 2
        R1, R2 = D1 // C, (D - D1) // C
        r = lax.axis_index('tp')
        grp = lax.axis_index('dp')
        z = r // C
        c = r % C
        gf = g.astype(f32)
        idf = ids.reshape(N)

        duf = du.reshape(N, FL)
        iota = jnp.arange(V, dtype=jnp.int32)

        Ep = lax.dynamic_slice_in_dim(E, grp * Vp, Vp, axis=0)
        AT = lax.all_gather(rows(Ep.T), 'tp', axis=0, tiled=True)

        du_o = lax.ppermute(duf, 'tp', swap)
        Ws = lax.dynamic_index_in_dim(W.reshape(Z, C, DL, FL), 1 - c, 1, False)
        W_o = lax.ppermute(Ws, 'tp', swap)
        el = E.astype(f32)
        ssl = jnp.sum(el * el, axis=1)
        ssl, _ = barrier((ssl, Ws))
        ssg = exchange(G, ssl.reshape(V // 128, 128))
        rs2 = lax.rsqrt(jnp.sum(ssg, axis=0) / D + EPS).reshape(1, V)
        gcol = gf.reshape(D, 1)
        du_o, W_o, gcol, rs2 = barrier((du_o, W_o, gcol, rs2))
        F = Z // 2

        streams = [(0, 1, F), (1, -1, F), (1, 1, F - 1), (0, -1, F - 1)]
        acc = {0: [], 1: []}

        def hop(bufs):
            out = {}
            for st, b in bufs.items():
                out[st] = lax.ppermute(b, 'tp', shift(st[1]))
            return out

        def blocks(k):
            return [(s * (L - k), h) for h, s, L in streams if k < L]

        def add(moved, k, parts, hook):
            nxt = {}
            for (h, s, L), b in moved.items():
                if k == L:
                    acc[h].append(b)
                else:
                    b, _ = barrier((b, hook))
                    nxt[(h, s, L)] = b.astype(f32) + parts[(s * (L - k), h)]
            return nxt

        def chip(bl, Wo, dtype):
            return chip_parts(bl, z, c, Z, C, duf, du_o, W, Wo, dtype)

        p = chip(blocks(0), W_o, bf16)
        bufs = {(h, s, L): p[(s * L, h)] for h, s, L in streams}
        moved = hop(bufs)
        Wo1, _ = barrier((W_o, tuple(bufs.values())))
        p2 = chip(blocks(1), Wo1, f32)

        b1 = lax.dynamic_slice_in_dim(AT, c * R1, R1, axis=0)
        b2 = lax.dynamic_slice_in_dim(AT, D1 + c * R2, R2, axis=0)
        b1, b2 = barrier((rows(b1), rows(b2)))
        e1 = lax.all_gather(b1, ('dp', 'tp'), axis_index_groups=groups, axis=0, tiled=False).reshape(DP, C, R1, Vp)
        e2 = lax.all_gather(b2, ('dp', 'tp'), axis_index_groups=groups, axis=0, tiled=False).reshape(DP, C, R2, Vp)

        bufs = add(moved, 1, p2, b2)
        Wo2, _ = barrier((W_o, tuple(bufs.values())))
        moved = hop(bufs)
        p3 = chip([t for k in range(2, F) for t in blocks(k)] + [(0, 0), (0, 1)], Wo2, f32)
        idx, _ = barrier((idf, tuple(p3.values())))
        dh, dl, xl = rowsums(idx.reshape(1, N), duf, E)
        rst = jnp.sum(jnp.where(idx[:, None] == iota[None, :], rs2, 0.0), axis=1)
        idr = lax.dynamic_slice_in_dim(ids, r * TL, TL, axis=1).reshape(K * TL)
        sr = (iota[:, None] == idr[None, :]).astype(bf16)
        idc = idf.reshape(N, 1)
        rs2, sr, idc, xl, rst = barrier((rs2, sr, idc, xl, rst))

        bufs = add(moved, 2, p3, xl)
        rs2, _ = barrier((rs2, tuple(bufs.values())))
        moved = hop(bufs)
        dw1, x1, up = forward(0, e1, rs2, gcol, W, dh, dl, sr)
        for k in range(3, F):
            bufs = add(moved, k, p3, up)
            rs2, _ = barrier((rs2, tuple(bufs.values())))
            moved = hop(bufs)
        drs, _ = barrier((dres, tuple(bufs.values())))
        dc = lax.all_to_all(drs.reshape(K, TL, G, DL), 'tp', 2, 0, tiled=False)
        dW, x2, u = forward(D1, e2, rs2, gcol, W, dh, dl, sr, up, idc, dw1, x1)
        moved = {st: barrier((b, u))[0] for st, b in moved.items()}
        dc, _ = barrier((dc, u))
        dresc = dc.reshape(G, K, TL, DL).transpose(1, 0, 2, 3).reshape(N, DL)
        add(moved, F, p3, u)
        dn = jnp.concatenate([p3[(0, h)] + sum(b.astype(f32) for b in acc[h]) for h in (0, 1)], axis=0)
        xo = x2.reshape(K, TL, D)
        u = u.reshape(K, T, FL)

        gl = lax.dynamic_slice_in_dim(gf, r * DL, DL)
        nh = xl.astype(f32) * rst[:, None]
        gdn = gl * dn
        sp = jnp.sum(nh * gdn, axis=1)
        dgl = jnp.sum(dn * nh, axis=0)
        small = jnp.concatenate([sp, dgl]).reshape((N + DL) // 128, 128)
        q = jnp.concatenate(split3(dresc.astype(f32) + rst[:, None] * gdn), axis=1)
        small, dA = tail(G, V, small, idx.reshape(1, N), q)
        small = small.reshape(G, N + DL)
        s = jnp.sum(small[:, :N], axis=0) / D
        dg = small[:, N:].reshape(D)
        sv = jnp.sum(jnp.where(iota[:, None] == idf[None, :], s[None, :], 0.0), axis=1)
        rv = rs2.reshape(V, 1)
        dE = dA - rv * (E.astype(f32) * rv) * sv[:, None]
        return u, xo, dE, dW, dg

    return jax.shard_map(
        program,
        mesh=mesh,
        in_specs=(P('dp', None), P(None, 'tp'), P(), P(None, 'tp'), P('dp', None, 'tp'), P('dp', 'tp', None)),
        out_specs=(P('dp', None, 'tp'), P('dp', 'tp', None), P('dp', 'tp'), P('dp', 'tp'), P('dp')),
        check_vma=False,
    )
```

```python
import functools

import jax
import jax.numpy as jnp
from jax import lax
from jax.experimental import pallas as pl
from jax.experimental.layout import Layout, with_layout_constraint
from jax.experimental.pallas import tpu as pltpu
from jax.sharding import PartitionSpec as P


EPS = 1e-6
MESH = pl.DeviceIdType.MESH
f32 = jnp.float32
bf16 = jnp.bfloat16


def parts_kernel(nb, idx_ref, a_ref, b_ref, wa_ref, wb_ref, *outs):
    nt = (((1,), (1,)), ((), ()))
    o = (lax.dot_general(a_ref[...], wa_ref[...], nt, preferred_element_type=f32)
         + lax.dot_general(b_ref[...], wb_ref[...], nt, preferred_element_type=f32)).astype(outs[0].dtype)
    for i in range(nb):
        @pl.when(pl.program_id(0) == i)
        def _(i=i):
            outs[i][...] = o


def chip_parts(blocks, z, c, Z, C, a, b, W, Wo, dtype):
    blocks = sorted(blocks, key=lambda t: t[1])
    nb = len(blocks)
    N, FL = a.shape
    DL = Wo.shape[1]
    M = N // 2
    zd = [lax.rem(z + d + Z, Z) for d, _ in blocks]
    idx = jnp.stack([q * C + c for q in zd] + zd)
    first = sum(1 for _, h in blocks if h == 0)
    row = lambda i, s: (jnp.where(i >= first, 1, 0), 0)
    outs = pl.pallas_call(
        functools.partial(parts_kernel, nb),
        grid_spec=pltpu.PrefetchScalarGridSpec(
            num_scalar_prefetch=1,
            grid=(nb,),
            in_specs=[
                pl.BlockSpec((M, FL), row), pl.BlockSpec((M, FL), row),
                pl.BlockSpec((DL, FL), lambda i, s: (s[i], 0)), pl.BlockSpec((DL, FL), lambda i, s: (s[nb + i], 0)),
            ],
            out_specs=[pl.BlockSpec((M, DL), lambda i, s: (0, 0)) for _ in blocks],
        ),
        out_shape=[jax.ShapeDtypeStruct((M, DL), dtype) for _ in blocks],
        cost_estimate=pl.CostEstimate(flops=4 * M * DL * FL * nb, bytes_accessed=8 << 20, transcendentals=0),
        compiler_params=pltpu.CompilerParams(dimension_semantics=("arbitrary",), vmem_limit_bytes=62 << 20),
        name="chip_parts",
    )(idx, a, b, W, Wo.reshape(-1, FL))
    return dict(zip(blocks, outs))


def adds_kernel(groups, *refs):
    n = sum(groups)
    i = 0
    for o, g in zip(refs[n:], groups):
        a = refs[i][...].astype(f32)
        for r in refs[i + 1:i + g]:
            a += r[...].astype(f32)
        o[...] = a
        i += g


def adds(terms):
    flat = [a for t in terms for a in t]
    M, L = flat[0].shape
    bm = 256
    spec = pl.BlockSpec((bm, L), lambda i: (i, 0))
    return pl.pallas_call(
        functools.partial(adds_kernel, tuple(len(t) for t in terms)),
        grid=(M // bm,),
        in_specs=[spec for _ in flat],
        out_specs=[spec for _ in terms],
        out_shape=[jax.ShapeDtypeStruct((M, L), f32) for _ in terms],
        cost_estimate=pl.CostEstimate(flops=1 << 28, bytes_accessed=4 * M * L * (len(flat) + len(terms)),
                                      transcendentals=0),
        compiler_params=pltpu.CompilerParams(dimension_semantics=("arbitrary",), vmem_limit_bytes=62 << 20),
        name="adds",
    )(*flat)


def rowsum_kernel(ids_ref, du_ref, e_ref, hi_ref, lo_ref, x_ref, acc_ref):
    i = pl.program_id(0)
    vb = e_ref.shape[0]
    hot = lax.broadcasted_iota(jnp.int32, (vb, du_ref.shape[0]), 0) + i * vb == ids_ref[...]
    hot = jnp.where(hot, 1.0, 0.0).astype(bf16)
    d = jnp.dot(hot, du_ref[...], preferred_element_type=f32)
    hi = d.astype(bf16)
    hi_ref[...] = hi
    lo_ref[...] = (d - hi.astype(f32)).astype(bf16)

    @pl.when(i == 0)
    def _():
        acc_ref[...] = jnp.zeros(acc_ref.shape, f32)

    acc_ref[...] += lax.dot_general(hot, e_ref[...], (((0,), (0,)), ((), ())), preferred_element_type=f32)

    @pl.when(i == pl.num_programs(0) - 1)
    def _():
        x_ref[...] = acc_ref[...].astype(bf16)


def rowsums(ids, du, E):
    N, FL = du.shape
    V, DL = E.shape
    vb = 512
    one = pl.Buffered(1)
    return pl.pallas_call(
        rowsum_kernel,
        grid=(V // vb,),
        in_specs=[
            pl.BlockSpec((1, N), lambda i: (0, 0)),
            pl.BlockSpec((N, FL), lambda i: (0, 0), pipeline_mode=one),
            pl.BlockSpec((vb, DL), lambda i: (i, 0)),
        ],
        out_specs=[pl.BlockSpec((vb, FL), lambda i: (i, 0)), pl.BlockSpec((vb, FL), lambda i: (i, 0)),
                   pl.BlockSpec((N, DL), lambda i: (0, 0))],
        out_shape=[pltpu.HBM((V, FL), bf16), pltpu.HBM((V, FL), bf16), pltpu.HBM((N, DL), bf16)],
        scratch_shapes=[pltpu.VMEM((N, DL), f32)],
        cost_estimate=pl.CostEstimate(flops=2 * V * N * (FL + DL), bytes_accessed=12 << 20, transcendentals=0),
        compiler_params=pltpu.CompilerParams(dimension_semantics=("arbitrary",), vmem_limit_bytes=30 << 20),
        name="rowsums",
    )(ids, du, E)


def send_all(G, s_ref, o_ref, send, recv):
    me = lax.axis_index('tp')
    bar = pltpu.get_barrier_semaphore()
    for k in range(1, G):
        pl.semaphore_signal(bar, inc=1, device_id={'tp': lax.rem(me + k, G)}, device_id_type=MESH)
    pl.semaphore_wait(bar, G - 1)
    copies = []
    for k in range(1, G):
        cp = pltpu.make_async_remote_copy(
            src_ref=s_ref, dst_ref=o_ref.at[me], send_sem=send.at[k - 1], recv_sem=recv.at[k - 1],
            device_id={'tp': lax.rem(me + k, G)}, device_id_type=MESH)
        cp.start()
        copies.append(cp)
    o_ref[me] = s_ref[...]
    return copies


def exchange_kernel(G, s_ref, o_ref, send, recv):
    for cp in send_all(G, s_ref, o_ref, send, recv):
        cp.wait()


def exchange(G, small):
    vm = pl.BlockSpec(memory_space=pltpu.VMEM)
    return pl.pallas_call(
        functools.partial(exchange_kernel, G),
        out_shape=jax.ShapeDtypeStruct((G,) + small.shape, f32),
        in_specs=[vm],
        out_specs=vm,
        scratch_shapes=[pltpu.SemaphoreType.DMA((G - 1,)), pltpu.SemaphoreType.DMA((G - 1,))],
        cost_estimate=pl.CostEstimate(flops=1 << 30, bytes_accessed=1 << 20, transcendentals=0),
        compiler_params=pltpu.CompilerParams(collective_id=1, has_side_effects=True, vmem_limit_bytes=4 << 20),
        name="exchange",
    )(small)


def tail_kernel(G, s_ref, ids_ref, q_ref, o_ref, d_ref, send, recv):
    copies = send_all(G, s_ref, o_ref, send, recv)
    N, Q = q_ref.shape
    DL = Q // 3
    vb = 512

    def block(i, carry):
        rows = pl.ds(pl.multiple_of(i * vb, vb), vb)
        hot = lax.broadcasted_iota(jnp.int32, (vb, N), 0) + i * vb == ids_ref[...]
        d3 = jnp.dot(jnp.where(hot, 1.0, 0.0).astype(bf16), q_ref[...], preferred_element_type=f32)
        d_ref[rows, :] = d3[:, :DL] + d3[:, DL:2 * DL] + d3[:, 2 * DL:]
        return carry

    lax.fori_loop(0, d_ref.shape[0] // vb, block, 0)
    for cp in copies:
        cp.wait()


def tail(G, V, small, ids, q):
    vm = pl.BlockSpec(memory_space=pltpu.VMEM)
    return pl.pallas_call(
        functools.partial(tail_kernel, G),
        out_shape=(jax.ShapeDtypeStruct((G,) + small.shape, f32), jax.ShapeDtypeStruct((V, q.shape[1] // 3), f32)),
        in_specs=[vm, vm, vm],
        out_specs=(vm, vm),
        scratch_shapes=[pltpu.SemaphoreType.DMA((G - 1,)), pltpu.SemaphoreType.DMA((G - 1,))],
        cost_estimate=pl.CostEstimate(flops=2 * V * q.shape[0] * q.shape[1], bytes_accessed=6 << 20, transcendentals=0),
        compiler_params=pltpu.CompilerParams(collective_id=0, has_side_effects=True, vmem_limit_bytes=40 << 20),
        name="tail",
    )(small, ids, q)


def forward_kernel(last, DP, *refs):
    if last:
        (eb_ref, rs_ref, g_ref, w_ref, dh_ref, dl_ref, sr_ref, up_ref, ids_ref, _, _,
         dw_ref, xo_ref, u_ref, acc_ref, n_ref) = refs
    else:
        (eb_ref, rs_ref, g_ref, w_ref, dh_ref, dl_ref, sr_ref, dw_ref, xo_ref, acc_ref, n_ref) = refs
    j = pl.program_id(0)
    kt, V = n_ref.shape

    @pl.when(j == 0)
    def _():
        acc_ref[...] = up_ref[...] if last else jnp.zeros(acc_ref.shape, f32)

    ck = 512
    for h in range(kt // ck):
        rows = slice(h * ck, (h + 1) * ck)
        x = jnp.concatenate([eb_ref[i, 0, rows, :] for i in range(DP)], axis=1)
        n_ref[rows, :] = (x.astype(f32) * rs_ref[...] * g_ref[rows, :]).astype(bf16)
        xo_ref[:, rows] = jnp.dot(x, sr_ref[...], preferred_element_type=f32).T.astype(bf16)
    dw_ref[...] = (jnp.dot(n_ref[...], dh_ref[...], preferred_element_type=f32)
                   + jnp.dot(n_ref[...], dl_ref[...], preferred_element_type=f32))
    acc_ref[...] += lax.dot_general(w_ref[...], n_ref[...], (((0,), (0,)), ((), ())), preferred_element_type=f32)

    if last:
        @pl.when(j == pl.num_programs(0) - 1)
        def _():
            FL = acc_ref.shape[0]
            n_ref[:FL, :] = acc_ref[...].astype(bf16)
            tb = 512

            def step(i, carry):
                rows = pl.ds(pl.multiple_of(i * tb, tb), tb)
                hot = lax.broadcasted_iota(jnp.int32, (tb, V), 1) == ids_ref[rows, :]
                s = jnp.where(hot, 1.0, 0.0).astype(bf16)
                u_ref[rows, :] = lax.dot_general(s, n_ref[:FL, :], (((1,), (1,)), ((), ())),
                                                 preferred_element_type=f32).astype(bf16)
                return carry

            lax.fori_loop(0, u_ref.shape[0] // tb, step, 0)


def forward(row0, eb, rs, gcol, W, dh, dl, sr, up=None, ids=None, dw=None, xo=None):
    last = up is not None
    DP, C, R, Vp = eb.shape
    V = DP * Vp
    D, FL = W.shape
    kt = 1024
    nk = R // kt
    TS = sr.shape[1]
    base = row0 // kt
    one = pl.Buffered(1)

    def full(shape):
        return pl.BlockSpec(shape, lambda j: (0,) * len(shape), pipeline_mode=one)

    in_specs = [
        pl.BlockSpec((DP, 1, kt, Vp), lambda j: (0, j // nk, j % nk, 0)),
        full((1, V)),
        pl.BlockSpec((kt, 1), lambda j: (base + j, 0)),
        pl.BlockSpec((kt, FL), lambda j: (base + j, 0)),
        full((V, FL)), full((V, FL)), full((V, TS)),
    ]
    args = [eb, rs, gcol, W, dh, dl, sr]
    out_shape = [jax.ShapeDtypeStruct((D, FL), f32), jax.ShapeDtypeStruct((TS, D), bf16)]
    out_specs = [pl.BlockSpec((kt, FL), lambda j: (base + j, 0)), pl.BlockSpec((TS, kt), lambda j: (0, base + j))]
    scratch = [pltpu.VMEM((kt, V), bf16)]
    alias = {}
    if last:
        N = ids.shape[0]
        in_specs += [full((FL, V)), full((N, 1)), pl.BlockSpec(memory_space=pl.ANY), pl.BlockSpec(memory_space=pl.ANY)]
        args += [up, ids, dw, xo]
        alias = {9: 0, 10: 1}
        out_shape.append(jax.ShapeDtypeStruct((N, FL), bf16))
        out_specs.append(full((N, FL)))
        scratch = [pltpu.VMEM((FL, V), f32)] + scratch
    else:
        out_shape.append(jax.ShapeDtypeStruct((FL, V), f32))
        out_specs.append(full((FL, V)))
    flops = 2 * V * FL * C * R * 3 + (2 * V * V * FL if last else 0)
    return pl.pallas_call(
        functools.partial(forward_kernel, last, DP),
        grid=(C * nk,),
        in_specs=in_specs,
        out_specs=out_specs,
        out_shape=out_shape,
        scratch_shapes=scratch,
        input_output_aliases=alias,
        cost_estimate=pl.CostEstimate(flops=flops, bytes_accessed=30 << 20, transcendentals=0),
        compiler_params=pltpu.CompilerParams(dimension_semantics=("arbitrary",), vmem_limit_bytes=62 << 20),
        name="forward",
    )(*args)


barrier = lax.optimization_barrier


def rows(a):
    return with_layout_constraint(a, Layout(major_to_minor=(0, 1)))


def split3(a):
    hi = lax.reduce_precision(a, 8, 7)
    mi = lax.reduce_precision(a - hi, 8, 7)
    lo = a - hi - mi
    return hi.astype(bf16), mi.astype(bf16), lo.astype(bf16)


def solution(mesh):
    G = mesh.shape['tp']
    DP = mesh.shape['dp']
    C = 2
    Z = G // C
    groups = [[d * G + z * C + c for d in range(DP) for c in range(C)] for z in range(Z)]

    def shift(k):
        return [(z * C + c, ((z + k) % Z) * C + c) for z in range(Z) for c in range(C)]

    swap = [(i, i ^ 1) for i in range(G)]

    def program(ids, E, g, W, du, dres):
        K, T = ids.shape
        N = K * T
        V, DL = E.shape
        D = g.shape[0]
        FL = W.shape[1]
        TL = T // G
        Vp = V // DP
        D1 = D // 2
        R1, R2 = D1 // C, (D - D1) // C
        r = lax.axis_index('tp')
        grp = lax.axis_index('dp')
        z = r // C
        c = r % C
        gf = g.astype(f32)
        idf = ids.reshape(N)

        duf = du.reshape(N, FL)
        iota = jnp.arange(V, dtype=jnp.int32)

        Ep = lax.dynamic_slice_in_dim(E, grp * Vp, Vp, axis=0)
        AT = lax.all_gather(rows(Ep.T), 'tp', axis=0, tiled=True)

        du_o = lax.ppermute(duf, 'tp', swap)
        Ws = lax.dynamic_index_in_dim(W.reshape(Z, C, DL, FL), 1 - c, 1, False)
        W_o = lax.ppermute(Ws, 'tp', swap)
        el = E.astype(f32)
        ssl = jnp.sum(el * el, axis=1)
        ssl, _ = barrier((ssl, Ws))
        ssg = exchange(G, ssl.reshape(V // 128, 128))
        rs2 = lax.rsqrt(jnp.sum(ssg, axis=0) / D + EPS).reshape(1, V)
        gcol = gf.reshape(D, 1)
        du_o, W_o, gcol, rs2 = barrier((du_o, W_o, gcol, rs2))
        F = Z // 2

        streams = [(0, 1, F), (1, -1, F), (1, 1, F - 1), (0, -1, F - 1)]
        acc = {0: [], 1: []}

        def hop(bufs):
            out = {}
            for st, b in bufs.items():
                out[st] = lax.ppermute(b, 'tp', shift(st[1]))
            return out

        def blocks(k):
            return [(s * (L - k), h) for h, s, L in streams if k < L]

        def add(moved, k, parts, hook):
            keys, terms = [], []
            for (h, s, L), b in moved.items():
                if k == L:
                    acc[h].append(b)
                else:
                    keys.append((h, s, L))
                    terms.append([b, parts[(s * (L - k), h)]])
            if not keys:
                return {}
            terms, _ = barrier((terms, hook))
            return dict(zip(keys, adds(terms)))

        def chip(bl, Wo, dtype):
            return chip_parts(bl, z, c, Z, C, duf, du_o, W, Wo, dtype)

        p = chip(blocks(0), W_o, bf16)
        bufs = {(h, s, L): p[(s * L, h)] for h, s, L in streams}
        moved = hop(bufs)
        Wo1, _ = barrier((W_o, tuple(bufs.values())))
        p2 = chip(blocks(1), Wo1, f32)

        b1 = lax.dynamic_slice_in_dim(AT, c * R1, R1, axis=0)
        b2 = lax.dynamic_slice_in_dim(AT, D1 + c * R2, R2, axis=0)
        b1, b2 = barrier((rows(b1), rows(b2)))
        e1 = lax.all_gather(b1, ('dp', 'tp'), axis_index_groups=groups, axis=0, tiled=False).reshape(DP, C, R1, Vp)
        e2 = lax.all_gather(b2, ('dp', 'tp'), axis_index_groups=groups, axis=0, tiled=False).reshape(DP, C, R2, Vp)

        bufs = add(moved, 1, p2, b2)
        Wo2, _ = barrier((W_o, tuple(bufs.values())))
        moved = hop(bufs)
        p3 = chip([t for k in range(2, F) for t in blocks(k)] + [(0, 0), (0, 1)], Wo2, f32)
        idx, _ = barrier((idf, tuple(p3.values())))
        dh, dl, xl = rowsums(idx.reshape(1, N), duf, E)
        rst = jnp.sum(jnp.where(idx[:, None] == iota[None, :], rs2, 0.0), axis=1)
        idr = lax.dynamic_slice_in_dim(ids, r * TL, TL, axis=1).reshape(K * TL)
        sr = (iota[:, None] == idr[None, :]).astype(bf16)
        idc = idf.reshape(N, 1)
        rs2, sr, idc, xl, rst = barrier((rs2, sr, idc, xl, rst))

        bufs = add(moved, 2, p3, xl)
        rs2, _ = barrier((rs2, tuple(bufs.values())))
        moved = hop(bufs)
        dw1, x1, up = forward(0, e1, rs2, gcol, W, dh, dl, sr)
        for k in range(3, F):
            bufs = add(moved, k, p3, up)
            rs2, _ = barrier((rs2, tuple(bufs.values())))
            moved = hop(bufs)
        drs, _ = barrier((dres, tuple(bufs.values())))
        dc = lax.all_to_all(drs.reshape(K, TL, G, DL), 'tp', 2, 0, tiled=False)
        dW, x2, u = forward(D1, e2, rs2, gcol, W, dh, dl, sr, up, idc, dw1, x1)
        moved = {st: barrier((b, u))[0] for st, b in moved.items()}
        dc, _ = barrier((dc, u))
        dresc = dc.reshape(G, K, TL, DL).transpose(1, 0, 2, 3).reshape(N, DL)
        add(moved, F, p3, u)
        dn = jnp.concatenate([p3[(0, h)] + sum(b.astype(f32) for b in acc[h]) for h in (0, 1)], axis=0)
        xo = x2.reshape(K, TL, D)
        u = u.reshape(K, T, FL)

        gl = lax.dynamic_slice_in_dim(gf, r * DL, DL)
        nh = xl.astype(f32) * rst[:, None]
        gdn = gl * dn
        sp = jnp.sum(nh * gdn, axis=1)
        dgl = jnp.sum(dn * nh, axis=0)
        small = jnp.concatenate([sp, dgl]).reshape((N + DL) // 128, 128)
        q = jnp.concatenate(split3(dresc.astype(f32) + rst[:, None] * gdn), axis=1)
        small, dA = tail(G, V, small, idx.reshape(1, N), q)
        small = small.reshape(G, N + DL)
        s = jnp.sum(small[:, :N], axis=0) / D
        dg = small[:, N:].reshape(D)
        sv = jnp.sum(jnp.where(iota[:, None] == idf[None, :], s[None, :], 0.0), axis=1)
        rv = rs2.reshape(V, 1)
        dE = dA - rv * (E.astype(f32) * rv) * sv[:, None]
        return u, xo, dE, dW, dg

    return jax.shard_map(
        program,
        mesh=mesh,
        in_specs=(P('dp', None), P(None, 'tp'), P(), P(None, 'tp'), P('dp', None, 'tp'), P('dp', 'tp', None)),
        out_specs=(P('dp', None, 'tp'), P('dp', 'tp', None), P('dp', 'tp'), P('dp', 'tp'), P('dp')),
        check_vma=False,
    )
```

```python
import functools

import jax
import jax.numpy as jnp
from jax import lax
from jax.experimental import pallas as pl
from jax.experimental.layout import Layout, with_layout_constraint
from jax.experimental.pallas import tpu as pltpu
from jax.sharding import PartitionSpec as P


EPS = 1e-6
MESH = pl.DeviceIdType.MESH
f32 = jnp.float32
bf16 = jnp.bfloat16


def parts_kernel(nb, idx_ref, a_ref, b_ref, wa_ref, wb_ref, *outs):
    nt = (((1,), (1,)), ((), ()))
    o = (lax.dot_general(a_ref[...], wa_ref[...], nt, preferred_element_type=f32)
         + lax.dot_general(b_ref[...], wb_ref[...], nt, preferred_element_type=f32)).astype(outs[0].dtype)
    for i in range(nb):
        @pl.when(pl.program_id(0) == i)
        def _(i=i):
            outs[i][...] = o


def chip_parts(blocks, z, c, Z, C, a, b, W, Wo, dtype):
    blocks = sorted(blocks, key=lambda t: t[1])
    nb = len(blocks)
    N, FL = a.shape
    DL = Wo.shape[1]
    M = N // 2
    zd = [lax.rem(z + d + Z, Z) for d, _ in blocks]
    idx = jnp.stack([q * C + c for q in zd] + zd)
    first = sum(1 for _, h in blocks if h == 0)
    row = lambda i, s: (jnp.where(i >= first, 1, 0), 0)
    outs = pl.pallas_call(
        functools.partial(parts_kernel, nb),
        grid_spec=pltpu.PrefetchScalarGridSpec(
            num_scalar_prefetch=1,
            grid=(nb,),
            in_specs=[
                pl.BlockSpec((M, FL), row), pl.BlockSpec((M, FL), row),
                pl.BlockSpec((DL, FL), lambda i, s: (s[i], 0)), pl.BlockSpec((DL, FL), lambda i, s: (s[nb + i], 0)),
            ],
            out_specs=[pl.BlockSpec((M, DL), lambda i, s: (0, 0)) for _ in blocks],
        ),
        out_shape=[jax.ShapeDtypeStruct((M, DL), dtype) for _ in blocks],
        cost_estimate=pl.CostEstimate(flops=4 * M * DL * FL * nb, bytes_accessed=8 << 20, transcendentals=0),
        compiler_params=pltpu.CompilerParams(dimension_semantics=("arbitrary",), vmem_limit_bytes=62 << 20),
        name="chip_parts",
    )(idx, a, b, W, Wo.reshape(-1, FL))
    return dict(zip(blocks, outs))


def adds_kernel(groups, *refs):
    n = sum(groups)
    i = 0
    for o, g in zip(refs[n:], groups):
        a = refs[i][...].astype(f32)
        for r in refs[i + 1:i + g]:
            a += r[...].astype(f32)
        o[...] = a
        i += g


def adds(terms):
    flat = [a for t in terms for a in t]
    M, L = flat[0].shape
    bm = 256
    spec = pl.BlockSpec((bm, L), lambda i: (i, 0))
    return pl.pallas_call(
        functools.partial(adds_kernel, tuple(len(t) for t in terms)),
        grid=(M // bm,),
        in_specs=[spec for _ in flat],
        out_specs=[spec for _ in terms],
        out_shape=[jax.ShapeDtypeStruct((M, L), f32) for _ in terms],
        cost_estimate=pl.CostEstimate(flops=1 << 28, bytes_accessed=4 * M * L * (len(flat) + len(terms)),
                                      transcendentals=0),
        compiler_params=pltpu.CompilerParams(dimension_semantics=("arbitrary",), vmem_limit_bytes=62 << 20),
        name="adds",
    )(*flat)


def rowsum_kernel(ids_ref, du_ref, e_ref, rs_ref, hi_ref, lo_ref, x_ref, rt_ref, acc_ref, hot_ref):
    i = pl.program_id(0)
    vb = e_ref.shape[0]
    hot = lax.broadcasted_iota(jnp.int32, (vb, du_ref.shape[0]), 0) + i * vb == ids_ref[...]
    hot_ref[...] = jnp.where(hot, 1.0, 0.0).astype(bf16)
    ck = 256

    def step(k, carry):
        cols = pl.ds(pl.multiple_of(k * ck, ck), ck)
        d = jnp.dot(hot_ref[...], du_ref[:, cols], preferred_element_type=f32)
        hi = d.astype(bf16)
        hi_ref[:, cols] = hi
        lo_ref[:, cols] = (d - hi.astype(f32)).astype(bf16)
        return carry

    lax.fori_loop(0, du_ref.shape[1] // ck, step, 0)

    @pl.when(i == 0)
    def _():
        acc_ref[...] = jnp.zeros(acc_ref.shape, f32)
        rt_ref[...] = jnp.zeros(rt_ref.shape, f32)

    acc_ref[...] += lax.dot_general(hot_ref[...], e_ref[...], (((0,), (0,)), ((), ())), preferred_element_type=f32)
    rt_ref[...] += jnp.dot(rs_ref[...], hot_ref[...], preferred_element_type=f32)

    @pl.when(i == pl.num_programs(0) - 1)
    def _():
        x_ref[...] = acc_ref[...].astype(bf16)


def rowsums(ids, du, E, rs3):
    N, FL = du.shape
    V, DL = E.shape
    vb = 512
    one = pl.Buffered(1)
    return pl.pallas_call(
        rowsum_kernel,
        grid=(V // vb,),
        in_specs=[
            pl.BlockSpec((1, N), lambda i: (0, 0)),
            pl.BlockSpec((N, FL), lambda i: (0, 0), pipeline_mode=one),
            pl.BlockSpec((vb, DL), lambda i: (i, 0)),
            pl.BlockSpec((rs3.shape[0], vb), lambda i: (0, i)),
        ],
        out_specs=[pl.BlockSpec((vb, FL), lambda i: (i, 0)), pl.BlockSpec((vb, FL), lambda i: (i, 0)),
                   pl.BlockSpec((N, DL), lambda i: (0, 0)), pl.BlockSpec((rs3.shape[0], N), lambda i: (0, 0))],
        out_shape=[pltpu.HBM((V, FL), bf16), pltpu.HBM((V, FL), bf16), pltpu.HBM((N, DL), bf16),
                   jax.ShapeDtypeStruct((rs3.shape[0], N), f32)],
        scratch_shapes=[pltpu.VMEM((N, DL), f32), pltpu.VMEM((vb, N), bf16)],
        cost_estimate=pl.CostEstimate(flops=2 * V * N * (FL + DL), bytes_accessed=12 << 20, transcendentals=0),
        compiler_params=pltpu.CompilerParams(dimension_semantics=("arbitrary",), vmem_limit_bytes=30 << 20),
        name="rowsums",
    )(ids, du, E, rs3)


def send_all(G, s_ref, o_ref, send, recv):
    me = lax.axis_index('tp')
    bar = pltpu.get_barrier_semaphore()
    for k in range(1, G):
        pl.semaphore_signal(bar, inc=1, device_id={'tp': lax.rem(me + k, G)}, device_id_type=MESH)
    pl.semaphore_wait(bar, G - 1)
    copies = []
    for k in range(1, G):
        cp = pltpu.make_async_remote_copy(
            src_ref=s_ref, dst_ref=o_ref.at[me], send_sem=send.at[k - 1], recv_sem=recv.at[k - 1],
            device_id={'tp': lax.rem(me + k, G)}, device_id_type=MESH)
        cp.start()
        copies.append(cp)
    o_ref[me] = s_ref[...]
    return copies


def exchange_kernel(G, s_ref, o_ref, send, recv):
    for cp in send_all(G, s_ref, o_ref, send, recv):
        cp.wait()


def exchange(G, small):
    vm = pl.BlockSpec(memory_space=pltpu.VMEM)
    return pl.pallas_call(
        functools.partial(exchange_kernel, G),
        out_shape=jax.ShapeDtypeStruct((G,) + small.shape, f32),
        in_specs=[vm],
        out_specs=vm,
        scratch_shapes=[pltpu.SemaphoreType.DMA((G - 1,)), pltpu.SemaphoreType.DMA((G - 1,))],
        cost_estimate=pl.CostEstimate(flops=1 << 30, bytes_accessed=1 << 20, transcendentals=0),
        compiler_params=pltpu.CompilerParams(collective_id=1, has_side_effects=True, vmem_limit_bytes=4 << 20),
        name="exchange",
    )(small)


def tail_kernel(G, s_ref, ids_ref, q_ref, o_ref, d_ref, send, recv):
    copies = send_all(G, s_ref, o_ref, send, recv)
    N, Q = q_ref.shape
    DL = Q // 3
    vb = 512

    def block(i, carry):
        rows = pl.ds(pl.multiple_of(i * vb, vb), vb)
        hot = lax.broadcasted_iota(jnp.int32, (vb, N), 0) + i * vb == ids_ref[...]
        d3 = jnp.dot(jnp.where(hot, 1.0, 0.0).astype(bf16), q_ref[...], preferred_element_type=f32)
        d_ref[rows, :] = d3[:, :DL] + d3[:, DL:2 * DL] + d3[:, 2 * DL:]
        return carry

    lax.fori_loop(0, d_ref.shape[0] // vb, block, 0)
    for cp in copies:
        cp.wait()


def tail(G, V, small, ids, q):
    vm = pl.BlockSpec(memory_space=pltpu.VMEM)
    return pl.pallas_call(
        functools.partial(tail_kernel, G),
        out_shape=(jax.ShapeDtypeStruct((G,) + small.shape, f32), jax.ShapeDtypeStruct((V, q.shape[1] // 3), f32)),
        in_specs=[vm, vm, vm],
        out_specs=(vm, vm),
        scratch_shapes=[pltpu.SemaphoreType.DMA((G - 1,)), pltpu.SemaphoreType.DMA((G - 1,))],
        cost_estimate=pl.CostEstimate(flops=2 * V * q.shape[0] * q.shape[1], bytes_accessed=6 << 20, transcendentals=0),
        compiler_params=pltpu.CompilerParams(collective_id=0, has_side_effects=True, vmem_limit_bytes=40 << 20),
        name="tail",
    )(small, ids, q)


def forward_kernel(last, DP, *refs):
    if last:
        (eb_ref, rs_ref, g_ref, w_ref, dh_ref, dl_ref, sr_ref, up_ref, ids_ref, _, _,
         dw_ref, xo_ref, u_ref, acc_ref, n_ref) = refs
    else:
        (eb_ref, rs_ref, g_ref, w_ref, dh_ref, dl_ref, sr_ref, dw_ref, xo_ref, acc_ref, n_ref) = refs
    j = pl.program_id(0)
    kt, V = n_ref.shape

    @pl.when(j == 0)
    def _():
        acc_ref[...] = up_ref[...] if last else jnp.zeros(acc_ref.shape, f32)

    ck = 512

    def tile(h, carry):
        rows = pl.ds(pl.multiple_of(h * ck, ck), ck)
        x = jnp.concatenate([eb_ref[i, 0, rows, :] for i in range(DP)], axis=1)
        n = (x.astype(f32) * rs_ref[...] * g_ref[rows, :]).astype(bf16)
        n_ref[rows, :] = n
        xo_ref[:, rows] = jnp.dot(x, sr_ref[...], preferred_element_type=f32).T.astype(bf16)
        dw_ref[rows, :] = (jnp.dot(n, dh_ref[...], preferred_element_type=f32)
                           + jnp.dot(n, dl_ref[...], preferred_element_type=f32))
        return carry

    lax.fori_loop(0, kt // ck, tile, 0)

    def lanes(h, carry):
        cols = pl.ds(pl.multiple_of(h * ck, ck), ck)
        acc_ref[:, cols] += lax.dot_general(w_ref[...], n_ref[:, cols], (((0,), (0,)), ((), ())),
                                            preferred_element_type=f32)
        return carry

    lax.fori_loop(0, V // ck, lanes, 0)

    if last:
        @pl.when(j == pl.num_programs(0) - 1)
        def _():
            FL = acc_ref.shape[0]
            n_ref[:FL, :] = acc_ref[...].astype(bf16)
            tb = 256

            def step(i, carry):
                rows = pl.ds(pl.multiple_of(i * tb, tb), tb)
                hot = lax.broadcasted_iota(jnp.int32, (tb, V), 1) == ids_ref[rows, :]
                s = jnp.where(hot, 1.0, 0.0).astype(bf16)
                u_ref[rows, :] = lax.dot_general(s, n_ref[:FL, :], (((1,), (1,)), ((), ())),
                                                 preferred_element_type=f32).astype(bf16)
                return carry

            lax.fori_loop(0, u_ref.shape[0] // tb, step, 0)


def forward(row0, eb, rs, gcol, W, dh, dl, sr, up=None, ids=None, dw=None, xo=None):
    last = up is not None
    DP, C, R, Vp = eb.shape
    V = DP * Vp
    D, FL = W.shape
    kt = 1024
    nk = R // kt
    TS = sr.shape[1]
    base = row0 // kt
    one = pl.Buffered(1)

    def full(shape):
        return pl.BlockSpec(shape, lambda j: (0,) * len(shape), pipeline_mode=one)

    in_specs = [
        pl.BlockSpec((DP, 1, kt, Vp), lambda j: (0, j // nk, j % nk, 0)),
        full((1, V)),
        pl.BlockSpec((kt, 1), lambda j: (base + j, 0)),
        pl.BlockSpec((kt, FL), lambda j: (base + j, 0)),
        full((V, FL)), full((V, FL)), full((V, TS)),
    ]
    args = [eb, rs, gcol, W, dh, dl, sr]
    out_shape = [jax.ShapeDtypeStruct((D, FL), f32), jax.ShapeDtypeStruct((TS, D), bf16)]
    out_specs = [pl.BlockSpec((kt, FL), lambda j: (base + j, 0)), pl.BlockSpec((TS, kt), lambda j: (0, base + j))]
    scratch = [pltpu.VMEM((kt, V), bf16)]
    alias = {}
    if last:
        N = ids.shape[0]
        in_specs += [full((FL, V)), full((N, 1)), pl.BlockSpec(memory_space=pl.ANY), pl.BlockSpec(memory_space=pl.ANY)]
        args += [up, ids, dw, xo]
        alias = {9: 0, 10: 1}
        out_shape.append(jax.ShapeDtypeStruct((N, FL), bf16))
        out_specs.append(full((N, FL)))
        scratch = [pltpu.VMEM((FL, V), f32)] + scratch
    else:
        out_shape.append(jax.ShapeDtypeStruct((FL, V), f32))
        out_specs.append(full((FL, V)))
    flops = 2 * V * FL * C * R * 3 + (2 * V * V * FL if last else 0)
    return pl.pallas_call(
        functools.partial(forward_kernel, last, DP),
        grid=(C * nk,),
        in_specs=in_specs,
        out_specs=out_specs,
        out_shape=out_shape,
        scratch_shapes=scratch,
        input_output_aliases=alias,
        cost_estimate=pl.CostEstimate(flops=flops, bytes_accessed=30 << 20, transcendentals=0),
        compiler_params=pltpu.CompilerParams(dimension_semantics=("arbitrary",), vmem_limit_bytes=62 << 20),
        name="forward",
    )(*args)


barrier = lax.optimization_barrier


def rows(a):
    return with_layout_constraint(a, Layout(major_to_minor=(0, 1)))


def split3(a):
    hi = lax.reduce_precision(a, 8, 7)
    mi = lax.reduce_precision(a - hi, 8, 7)
    lo = a - hi - mi
    return hi.astype(bf16), mi.astype(bf16), lo.astype(bf16)


def solution(mesh):
    G = mesh.shape['tp']
    DP = mesh.shape['dp']
    C = 2
    Z = G // C
    groups = [[d * G + z * C + c for d in range(DP) for c in range(C)] for z in range(Z)]

    def shift(k):
        return [(z * C + c, ((z + k) % Z) * C + c) for z in range(Z) for c in range(C)]

    swap = [(i, i ^ 1) for i in range(G)]

    def program(ids, E, g, W, du, dres):
        K, T = ids.shape
        N = K * T
        V, DL = E.shape
        D = g.shape[0]
        FL = W.shape[1]
        TL = T // G
        Vp = V // DP
        D1 = D // 2
        R1, R2 = D1 // C, (D - D1) // C
        r = lax.axis_index('tp')
        grp = lax.axis_index('dp')
        z = r // C
        c = r % C
        gf = g.astype(f32)
        idf = ids.reshape(N)

        duf = du.reshape(N, FL)
        iota = jnp.arange(V, dtype=jnp.int32)

        Ep = lax.dynamic_slice_in_dim(E, grp * Vp, Vp, axis=0)
        AT = lax.all_gather(rows(Ep.T), 'tp', axis=0, tiled=True)

        du_o = lax.ppermute(duf, 'tp', swap)
        Ws = lax.dynamic_index_in_dim(W.reshape(Z, C, DL, FL), 1 - c, 1, False)
        W_o = lax.ppermute(Ws, 'tp', swap)
        el = E.astype(f32)
        ssl = jnp.sum(el * el, axis=1)
        ssl, _ = barrier((ssl, Ws))
        ssg = exchange(G, ssl.reshape(V // 128, 128))
        rs2 = lax.rsqrt(jnp.sum(ssg, axis=0) / D + EPS).reshape(1, V)
        gcol = gf.reshape(D, 1)
        du_o, W_o, gcol, rs2 = barrier((du_o, W_o, gcol, rs2))
        F = Z // 2

        streams = [(0, 1, F), (1, -1, F), (1, 1, F - 1), (0, -1, F - 1)]
        acc = {0: [], 1: []}

        def hop(bufs):
            out = {}
            for st, b in bufs.items():
                out[st] = lax.ppermute(b, 'tp', shift(st[1]))
            return out

        def blocks(k):
            return [(s * (L - k), h) for h, s, L in streams if k < L]

        def add(moved, k, parts, hook):
            keys, terms = [], []
            for (h, s, L), b in moved.items():
                if k == L:
                    acc[h].append(b)
                else:
                    keys.append((h, s, L))
                    terms.append([b, parts[(s * (L - k), h)]])
            if not keys:
                return {}
            terms, _ = barrier((terms, hook))
            return dict(zip(keys, adds(terms)))

        def chip(bl, Wo, dtype):
            return chip_parts(bl, z, c, Z, C, duf, du_o, W, Wo, dtype)

        p = chip(blocks(0), W_o, bf16)
        bufs = {(h, s, L): p[(s * L, h)] for h, s, L in streams}
        moved = hop(bufs)
        Wo1, _ = barrier((W_o, tuple(bufs.values())))
        p2 = chip(blocks(1), Wo1, f32)

        b1 = lax.dynamic_slice_in_dim(AT, c * R1, R1, axis=0)
        b2 = lax.dynamic_slice_in_dim(AT, D1 + c * R2, R2, axis=0)
        b1, b2 = barrier((rows(b1), rows(b2)))
        e1 = lax.all_gather(b1, ('dp', 'tp'), axis_index_groups=groups, axis=0, tiled=False).reshape(DP, C, R1, Vp)
        e2 = lax.all_gather(b2, ('dp', 'tp'), axis_index_groups=groups, axis=0, tiled=False).reshape(DP, C, R2, Vp)

        bufs = add(moved, 1, p2, b2)
        Wo2, _ = barrier((W_o, tuple(bufs.values())))
        moved = hop(bufs)
        p3 = chip([t for k in range(2, F) for t in blocks(k)] + [(0, 0), (0, 1)], Wo2, f32)
        idx, _ = barrier((idf, tuple(p3.values())))
        rs3 = jnp.concatenate(list(split3(rs2)) + [jnp.zeros((5, V), bf16)], axis=0)
        dh, dl, xl, rt = rowsums(idx.reshape(1, N), duf, E, rs3)
        rst = rt[0] + rt[1] + rt[2]
        idr = lax.dynamic_slice_in_dim(ids, r * TL, TL, axis=1).reshape(K * TL)
        sr = (iota[:, None] == idr[None, :]).astype(bf16)
        idc = idf.reshape(N, 1)
        rs2, sr, idc, xl, rst = barrier((rs2, sr, idc, xl, rst))

        bufs = add(moved, 2, p3, xl)
        rs2, _ = barrier((rs2, tuple(bufs.values())))
        moved = hop(bufs)
        dw1, x1, up = forward(0, e1, rs2, gcol, W, dh, dl, sr)
        for k in range(3, F):
            bufs = add(moved, k, p3, up)
            rs2, _ = barrier((rs2, tuple(bufs.values())))
            moved = hop(bufs)
        drs, _ = barrier((dres, tuple(bufs.values())))
        dc = lax.all_to_all(drs.reshape(K, TL, G, DL), 'tp', 2, 0, tiled=False)
        dW, x2, u = forward(D1, e2, rs2, gcol, W, dh, dl, sr, up, idc, dw1, x1)
        moved = {st: barrier((b, u))[0] for st, b in moved.items()}
        dc, _ = barrier((dc, u))
        dresc = dc.reshape(G, K, TL, DL).transpose(1, 0, 2, 3).reshape(N, DL)
        add(moved, F, p3, u)
        dn = jnp.concatenate([p3[(0, h)] + sum(b.astype(f32) for b in acc[h]) for h in (0, 1)], axis=0)
        xo = x2.reshape(K, TL, D)
        u = u.reshape(K, T, FL)

        gl = lax.dynamic_slice_in_dim(gf, r * DL, DL)
        nh = xl.astype(f32) * rst[:, None]
        gdn = gl * dn
        sp = jnp.sum(nh * gdn, axis=1)
        dgl = jnp.sum(dn * nh, axis=0)
        small = jnp.concatenate([sp, dgl]).reshape((N + DL) // 128, 128)
        q = jnp.concatenate(split3(dresc.astype(f32) + rst[:, None] * gdn), axis=1)
        small, dA = tail(G, V, small, idx.reshape(1, N), q)
        small = small.reshape(G, N + DL)
        s = jnp.sum(small[:, :N], axis=0) / D
        dg = small[:, N:].reshape(D)
        sv = jnp.sum(jnp.where(iota[:, None] == idf[None, :], s[None, :], 0.0), axis=1)
        rv = rs2.reshape(V, 1)
        dE = dA - rv * (E.astype(f32) * rv) * sv[:, None]
        return u, xo, dE, dW, dg

    return jax.shard_map(
        program,
        mesh=mesh,
        in_specs=(P('dp', None), P(None, 'tp'), P(), P(None, 'tp'), P('dp', None, 'tp'), P('dp', 'tp', None)),
        out_specs=(P('dp', None, 'tp'), P('dp', 'tp', None), P('dp', 'tp'), P('dp', 'tp'), P('dp')),
        check_vma=False,
    )
```
